32 devices in a mesh: tm: 8 (over z, y), space: 4 (over x, core).
Axes of the slice: x: 2, y: 2, z: 4, core: 2. Of those that a mesh axis runs over, the one named last changes fastest.
Arguments:
- source: float32 [8, 32, 128, 128], P('tm', 'space'), may hold values from -8 to 8
- conductivity: float32 [32, 128, 128], P('space'), may hold values from 0.5 to 4
Outputs:
- solution: float32 [8, 32, 128, 128], P('tm', 'space')
- final_defect: float32 [8, 32, 128, 128], P('tm', 'space')
The draws below stay inside these ranges and needn't reach their ends.
All inputs are finite; a program needn't handle non-finite values.
Results may differ from the reference program's by a relative error of at most 0.000034.
Values sent between devices are 32-bit elements; how exact they have to be, the bound alone decides.
A program may use at most 64 MiB of HBM per device.

```python
import math
import jax
import jax.numpy as jnp

NX = 128
NY = 128
NU = 2
NC = 4
NZ = 32
NT = 8


def level_of(rng, extent, split, smallest, high):
    gain, own = 1.0, jax.random.fold_in(rng, 6)
    for position, parts in split:
        draws = jnp.exp(jax.random.uniform(jax.random.fold_in(own, position), (parts,), jnp.float32, smallest / len(split), high / len(split)))
        gain = gain * jnp.repeat(draws, extent[position] // parts).reshape([-1 if axis == position else 1 for axis in range(len(extent))])
    return gain


def normal_values(key, extent, spread, reach, split=(), held_as=jnp.bfloat16):
    drawn = jax.random.normal(key, extent, jnp.float32) * spread
    if len(split) > 0:
        drawn = level_of(key, extent, split, -0.22, 0.18) * drawn
    return jnp.clip(drawn, min=-reach, max=reach).astype(held_as)


def setup_inputs(seed: int = 0) -> dict:
    key_of = jax.random.split(jax.random.key(seed), 3)
    source = normal_values(key_of[0], (NT, NZ, NX, NY), 1.0, 8.0, ((0, 8), (1, 4)), jnp.float32)
    conductivity = jnp.clip(jnp.exp(math.log(4.0) - 2.0794415 * jax.random.uniform(key_of[1], (NZ, NX, NY), jnp.float32) ** level_of(key_of[1], (NZ, NX, NY), ((0, 4),), -0.2, 0.2)), 0.5, 4.0)
    return {"source": source, "conductivity": conductivity}


OMEGA = 0.8
FINE = (1.0, 1.0, 1.0)
COARSE = (0.25, 0.25, 1.0)


def stencil(padded, weights):
    weight_z, weight_x, weight_y = weights
    centre = padded[..., 1:-1, :, :]
    widths = [(0, 0)] * (centre.ndim - 2) + [(1, 1), (1, 1)]
    framed = jnp.pad(centre, widths)
    along_z = 2.0 * centre - padded[..., 2:, :, :] - padded[..., :-2, :, :]
    along_x = 2.0 * centre - framed[..., 2:, 1:-1] - framed[..., :-2, 1:-1]
    along_y = 2.0 * centre - framed[..., 1:-1, 2:] - framed[..., 1:-1, :-2]
    return weight_z * along_z + weight_x * along_x + weight_y * along_y


def defect(current, right_side, earlier, padded, conduct, stretch, weights):
    applied = current + stretch * conduct * stencil(padded, weights)
    return right_side + earlier - applied


def relaxed(current, right_side, earlier, padded, conduct, stretch, weights):
    weight_sum = 2.0 * (weights[0] + weights[1] + weights[2])
    diagonal = 1.0 + stretch * conduct * weight_sum
    return current + OMEGA * defect(current, right_side, earlier, padded, conduct, stretch, weights) / diagonal


def coarsen(values):
    return 0.25 * ((values[..., 0::2, 0::2, :] + values[..., 1::2, 0::2, :]) + (values[..., 0::2, 1::2, :] + values[..., 1::2, 1::2, :]))


def refine(values):
    return jnp.repeat(jnp.repeat(values, 2, axis=-3), 2, axis=-2)


def pad_planes(values):
    return jnp.pad(values, [(0, 0)] * (values.ndim - 3) + [(1, 1), (0, 0), (0, 0)])


def time_before(values):
    return jnp.concatenate([jnp.zeros_like(values[:1]), values[:-1]], 0)


def smooth(current, right_side, conduct, stretch, weights, repeats):
    for turn_index in range(repeats):
        current = relaxed(current, right_side, time_before(current), pad_planes(current), conduct, stretch, weights)
    return current


def level_defect(current, right_side, conduct, stretch, weights):
    return defect(current, right_side, time_before(current), pad_planes(current), conduct, stretch, weights)


def reference(source, conductivity):
    solution = smooth(jnp.zeros_like(source), source, conductivity, 1.0, FINE, NU)
    defect_fine = level_defect(solution, source, conductivity, 1.0, FINE)
    middle_rhs = defect_fine[0::2] + defect_fine[1::2]
    middle = smooth(jnp.zeros_like(middle_rhs), middle_rhs, conductivity, 2.0, FINE, NU)
    middle_defect = level_defect(middle, middle_rhs, conductivity, 2.0, FINE)
    summed = middle_defect[0::2] + middle_defect[1::2]
    coarse_rhs = coarsen(summed)
    coarse_cond = coarsen(conductivity)
    coarse = smooth(jnp.zeros_like(coarse_rhs), coarse_rhs, coarse_cond, 4.0, COARSE, NC)
    middle = middle + jnp.repeat(refine(coarse), 2, axis=0)
    middle = smooth(middle, middle_rhs, conductivity, 2.0, FINE, NU)
    solution = solution + jnp.repeat(middle, 2, axis=0)
    solution = smooth(solution, source, conductivity, 1.0, FINE, NU)
    final_defect = level_defect(solution, source, conductivity, 1.0, FINE)
    return solution, final_defect
```

```python
import functools

import jax
import jax.numpy as jnp
from jax import lax
from jax.experimental import pallas as pl
from jax.experimental.pallas import tpu as pltpu
from jax.sharding import PartitionSpec as P

NU = 2
NC = 4


OMEGA = 0.8
FINE = (1.0, 1.0, 1.0)
COARSE = (0.25, 0.25, 1.0)


def padded_2(shard, sides, width):
    for axis, dim in sides:
        peers, length = (lax.axis_size(axis), shard.shape[dim])
        up = [(i, (i + 1) % peers) for i in range(peers - 1)]
        down = [(j, i) for i, j in up]
        last = lax.slice_in_dim(shard, length - width, length, axis=dim)
        first = lax.slice_in_dim(shard, 0, width, axis=dim)
        before = lax.ppermute(last, axis, up)
        after = lax.ppermute(first, axis, down)
        shard = jnp.concatenate([before, shard, after], axis=dim)
    return shard


def shifted(shard, axis, by):
    peers = lax.axis_size(axis)
    pairs = [(i, i + by) for i in range(peers) if 0 <= i + by < peers]
    return lax.ppermute(shard, axis, pairs)


def swapped(value, axis, bit):
    mask = 2**bit
    pairs = [(source, source ^ mask) for source in range(lax.axis_size(axis))]
    return lax.ppermute(value, axis, pairs)


def stencil(padded, weights):
    weight_z, weight_x, weight_y = weights
    centre = padded[1:-1, :, 1:-1]
    widened = jnp.pad(padded[1:-1], ((0, 0), (1, 1), (0, 0)))
    along_z = 2.0 * centre - padded[2:, :, 1:-1] - padded[:-2, :, 1:-1]
    along_x = 2.0 * centre - widened[:, 2:, 1:-1] - widened[:, :-2, 1:-1]
    along_y = 2.0 * centre - padded[1:-1, :, 2:] - padded[1:-1, :, :-2]
    return weight_z * along_z + weight_x * along_x + weight_y * along_y


def defect(current, right_side, earlier, padded, conduct, stretch, weights):
    applied = current + stretch * conduct * stencil(padded, weights)
    return right_side + earlier - applied


def relaxed(current, right_side, earlier, padded, conduct, stretch, weights):
    weight_sum = 2.0 * (weights[0] + weights[1] + weights[2])
    diagonal = 1.0 + stretch * conduct * weight_sum
    return (
        current
        + OMEGA * defect(current, right_side, earlier, padded, conduct, stretch, weights) / diagonal
    )


def coarsen(values):
    return 0.25 * (
        values[..., 0::2, 0::2, :]
        + values[..., 1::2, 0::2, :]
        + (values[..., 0::2, 1::2, :] + values[..., 1::2, 1::2, :])
    )


def refine(values):
    return jnp.repeat(jnp.repeat(values, 2, axis=-3), 2, axis=-2)


def zero_columns(values):
    return jnp.pad(values, ((0, 0), (0, 0), (1, 1)))


def plane_faces(values):
    return padded_2(values, (("space", 0),), 1)


def coarse_planes_framed(values):
    return padded_2(values, (("space", 0),), 1)


def fine_frame(values):
    return zero_columns(plane_faces(values))


def step_prior(values):
    return shifted(values, "tm", 1)


def pair_prior(values):
    return shifted(values, "tm", 2)


def group_prior(values):
    return shifted(values, "tm", 4)


def smooth(current, right_side, conduct, stretch, weights, repeats, earlier_of, framing):
    for turn_index in range(repeats):
        current = relaxed(
            current, right_side, earlier_of(current), framing(current), conduct, stretch, weights
        )
    return current


def body(source, conductivity):
    right_side = source[0]
    solution = smooth(
        jnp.zeros_like(right_side), right_side, conductivity, 1.0, FINE, NU, step_prior, fine_frame
    )
    defect_fine = defect(
        solution, right_side, step_prior(solution), fine_frame(solution), conductivity, 1.0, FINE
    )
    middle_full = defect_fine + swapped(defect_fine, "tm", 0)
    middle = smooth(
        jnp.zeros_like(middle_full),
        middle_full,
        conductivity,
        2.0,
        FINE,
        NU,
        pair_prior,
        fine_frame,
    )
    middle_defect = defect(
        middle, middle_full, pair_prior(middle), fine_frame(middle), conductivity, 2.0, FINE
    )
    summed = middle_defect + swapped(middle_defect, "tm", 1)
    coarse_rhs = coarsen(summed)
    coarse_cond = coarsen(conductivity)

    def coarse_frame(values):
        return zero_columns(coarse_planes_framed(values))

    coarse = smooth(
        jnp.zeros_like(coarse_rhs),
        coarse_rhs,
        coarse_cond,
        4.0,
        COARSE,
        NC,
        group_prior,
        coarse_frame,
    )
    middle = middle + refine(coarse)
    middle = smooth(middle, middle_full, conductivity, 2.0, FINE, NU, pair_prior, fine_frame)
    solution = solution + middle
    solution = smooth(solution, right_side, conductivity, 1.0, FINE, NU, step_prior, fine_frame)
    final_defect = defect(
        solution, right_side, step_prior(solution), fine_frame(solution), conductivity, 1.0, FINE
    )
    return (solution[None], final_defect[None])


MESH = pl.DeviceIdType.MESH


def snake(index):
    return index + ((index // 2) % 2) * (1 - 2 * (index % 2))


def scaled(weights, stretch):
    return tuple(stretch * weight for weight in weights)


def fits(steps, peers, slabs, planes, rows, lanes):
    block = rows // peers
    return (
        steps == peers
        and peers % 8 == 0
        and peers & (peers - 1) == 0
        and rows % peers == 0
        and block % 8 == 0
        and planes % 2 == 0
        and planes >= 8
        and lanes % 128 == 0
        and peers == 8
        and slabs > 1
    )


PAD, PAD2 = 3, 4
NEAR = 2 * PAD2
UNROLL = 24


def cycle_kernel(
    peers,
    slabs,
    source_far,
    conduct_far,
    out_solution,
    out_defect,
    rhs, rhs1, rhs2, scrap,
    cond, gain0, hold0, gain1, hold1, gain2, hold2,
    a1, a2, a3, a4, a5, fd,
    m1, m2, m3, m4, m5,
    k1, k2, k3, k4,
    source,
    in_send, in_recv, own_sem, load_sem, cond_load,
    cond_send, cond_recv,
    h_send, h_recv,
    out_send, out_recv, out_own,
):
    planes, rows, lanes = source.shape
    block = rows // peers
    half_planes, half_block = planes // 2, block // 2
    me, slab = lax.axis_index("tm"), lax.axis_index("space")
    mine = snake(me)
    following, preceding = snake((mine + 1) % peers), snake((mine + peers - 1) % peers)
    has_z = {1: slab < slabs - 1, -1: slab > 0, 0: None}
    has_x = {1: mine < peers - 1, -1: mine > 0, 0: None}
    beside = {1: following, -1: preceding}

    def both(first, second):
        if first is None:
            return second
        return first if second is None else first & second

    def device(dz, dx):
        where = {}
        if dx:
            where["tm"] = beside[dx]
        if dz:
            where["space"] = slab + dz
        return where

    def size_of(ref):
        pad = PAD2 if ref.shape[0] == half_planes + 2 * PAD2 else PAD
        return pad, ref.shape[0] - 2 * pad, ref.shape[1] - 2 * pad

    def over(ref, outer, inner, work):
        pad, depth, width = size_of(ref)
        z0, z1, x0, x1 = pad - outer, pad + depth + outer, pad - outer, pad + width + outer
        parts = []
        if inner is None:
            parts.append((z0, z1, list(range(x0, x1))))
        else:
            i0, i1, j0, j1 = pad - inner, pad + depth + inner, pad - inner, pad + width + inner
            parts.append((z0, i0, list(range(x0, x1))))
            parts.append((i1, z1, list(range(x0, x1))))
            parts.append((i0, i1, list(range(x0, j0)) + list(range(j1, x1))))
        for first, last, xs in parts:
            count = last - first
            if count <= 0 or not xs:
                continue
            folds = [u for u in range(1, count + 1) if count % u == 0 and u * len(xs) <= UNROLL]
            fold = max(folds) if folds else 1
            if fold == count:
                for z in range(first, last):
                    work(z, xs)
                continue

            def step(i, _, first=first, xs=xs, fold=fold):
                for u in range(fold):
                    work(first + i * fold + u, xs)
                return 0

            lax.fori_loop(0, count // fold, step, 0)

    load_source = pltpu.make_async_copy(source_far, source, load_sem)
    load_source.start()

    def window(number):
        start, count, at = ((0, block, NEAR), (-NEAR, NEAR, 0), (block, NEAR, NEAR + block))[number]
        return pltpu.make_async_copy(
            conduct_far.at[:, pl.ds(pl.multiple_of(mine * block + start, 8), count), :],
            cond.at[pl.ds(NEAR, planes), pl.ds(at, count), :],
            cond_load.at[number],
        )

    window(0).start()
    pl.when(has_x[-1])(window(1).start)
    pl.when(has_x[1])(window(2).start)

    barrier = pltpu.get_barrier_semaphore()
    for k in range(1, peers):
        pl.semaphore_signal(barrier, inc=1, device_id={"tm": me ^ k}, device_id_type=MESH)
    expected = peers - 1
    for dz in (1, -1):
        for dx in (0, 1, -1):
            here = both(has_z[dz], has_x[dx])

            @pl.when(here)
            def _(dz=dz, dx=dx):
                pl.semaphore_signal(
                    barrier, inc=1, device_id=device(dz, dx), device_id_type=MESH
                )

            expected = expected + jnp.where(here, 1, 0)
    load_source.wait()
    pl.semaphore_wait(barrier, expected)

    def rows_of(index):
        return pl.ds(pl.multiple_of(snake(index) * block, 8), block)

    def inward(peer, step, recv):
        return pltpu.make_async_remote_copy(
            src_ref=source.at[:, rows_of(peer), :],
            dst_ref=rhs.at[pl.ds(PAD, planes), pl.ds(PAD, block), step, :],
            send_sem=in_send.at[peer],
            recv_sem=in_recv.at[recv],
            device_id={"tm": peer},
            device_id_type=MESH,
        )

    order = sorted(range(1, peers), reverse=True)
    for k in order:
        inward(me ^ k, me, me).start()
    own = pltpu.make_async_copy(
        source_far.at[:, rows_of(me), :],
        rhs.at[pl.ds(PAD, planes), pl.ds(PAD, block), me, :],
        own_sem,
    )
    own.start()
    window(0).wait()
    pl.when(has_x[-1])(window(1).wait)
    pl.when(has_x[1])(window(2).wait)

    def cond_copy(side, dz):
        return pltpu.make_async_remote_copy(
            src_ref=cond.at[pl.ds(planes, NEAR) if dz > 0 else pl.ds(NEAR, NEAR)],
            dst_ref=cond.at[pl.ds(0, NEAR) if dz > 0 else pl.ds(NEAR + planes, NEAR)],
            send_sem=cond_send.at[side],
            recv_sem=cond_recv.at[side],
            device_id={"space": slab + dz},
            device_id_type=MESH,
        )

    for side, dz in ((0, 1), (1, -1)):
        pl.when(has_z[dz])(cond_copy(side, dz).start)

    for ref in (rhs, rhs1, a3, m3, m5, rhs2):
        pad, deep, broad = size_of(ref)
        for dz, first in ((-1, 0), (1, pad + deep)):

            @pl.when(jnp.logical_not(has_z[dz]))
            def _(ref=ref, first=first, pad=pad):
                def clear(z, _):
                    ref[z] = jnp.zeros(ref.shape[1:], jnp.float32)
                    return 0

                lax.fori_loop(first, first + pad, clear, 0)

        for dx, first in ((-1, 0), (1, pad + broad)):

            @pl.when(jnp.logical_not(has_x[dx]))
            def _(ref=ref, first=first, pad=pad):
                def clear(z, _):
                    ref[z, first : first + pad] = jnp.zeros((pad, peers, lanes), jnp.float32)
                    return 0

                lax.fori_loop(0, ref.shape[0], clear, 0)

    for side, dz in ((0, 1), (1, -1)):
        pl.when(has_z[-dz])(cond_copy(side, dz).wait_recv)

    def fill(z, _):
        plane = slab * planes + z - PAD
        deep = (plane >= 0) & (plane < slabs * planes)
        for part in range((block + 2 * NEAR) // 8):
            at = pl.ds(8 * part, 8)
            row = mine * block - NEAR + 8 * part + lax.broadcasted_iota(jnp.int32, (8, lanes), 0)
            ok = deep & (row >= 0) & (row < rows)
            value = jnp.where(ok, cond[z - PAD + NEAR, at, :], 0.0)
            fine = jnp.where(ok, OMEGA / (1.0 + value * (2.0 * sum(FINE))), 0.0)
            middle = jnp.where(ok, OMEGA / (1.0 + value * (4.0 * sum(FINE))), 0.0)
            gain0[z, at, :] = fine
            hold0[z, at, :] = fine * value
            gain1[z, at, :] = middle
            hold1[z, at, :] = middle * (2.0 * value)
        return 0

    lax.fori_loop(0, planes + 2 * PAD, fill, 0)

    def fill2(z, _):
        plane = slab * half_planes + z - PAD2
        deep = (plane >= 0) & (plane < slabs * half_planes)
        for part in range((block + 2 * NEAR) // 16):
            at = pl.ds(8 * part, 8)
            even, odd = pl.ds(16 * part, 8, stride=2), pl.ds(16 * part + 1, 8, stride=2)
            quad = (cond[2 * z, even, :] + cond[2 * z + 1, even, :]) + (
                cond[2 * z, odd, :] + cond[2 * z + 1, odd, :]
            )
            row = mine * half_block - PAD2 + 8 * part
            row = row + lax.broadcasted_iota(jnp.int32, (8, lanes), 0)
            ok = deep & (row >= 0) & (row < rows // 2)
            value = jnp.where(ok, 0.25 * quad, 0.0)
            gain = jnp.where(ok, OMEGA / (1.0 + value * (8.0 * sum(COARSE))), 0.0)
            gain2[z, at, :] = gain
            hold2[z, at, :] = gain * value
        return 0

    lax.fori_loop(0, half_planes + 2 * PAD2, fill2, 0)

    time = lax.broadcasted_iota(jnp.int32, (peers, lanes), 0)
    lane = lax.broadcasted_iota(jnp.int32, (peers, lanes), 1)
    not_first, not_last = lane > 0, lane < lanes - 1
    later = {count: time % count > 0 for count in (peers, peers // 2, peers // 4)}

    def pick(value, index):
        return jnp.take_along_axis(value, index, axis=0, mode="promise_in_bounds")

    def prior(value, steps):
        return jnp.where(later[steps], pltpu.roll(value, 1, 0), 0.0)

    def spread(ref, z, x, pad):
        near = PAD2 if pad == PAD2 else NEAR
        return jnp.broadcast_to(ref[z, pl.ds(x - pad + near, 1), :], (peers, lanes))

    def around(ref, z, xs, weight_y):
        wanted = sorted({x + step for x in xs for step in (-1, 0, 1)})
        row = {x: ref[z, x] for x in wanted}
        for x in xs:
            centre = row[x]
            across = (ref[z - 1, x] + ref[z + 1, x]) + (row[x - 1] + row[x + 1])
            along = jnp.where(not_first, pltpu.roll(centre, 1, 1), 0.0) + jnp.where(
                not_last, pltpu.roll(centre, lanes - 1, 1), 0.0
            )
            total = across + along if weight_y == 1.0 else across + weight_y * along
            yield x, centre, total

    def sweeper(new, old, first, gain, hold, steps, weight_y=1.0):
        pad = size_of(new)[0]

        def work(z, xs):
            for x, centre, total in around(old, z, xs, weight_y):
                if first is None:
                    value = (2.0 - OMEGA) * centre
                else:
                    value = (1.0 - OMEGA) * centre + first[z, x]
                value = value + spread(gain, z, x, pad) * prior(centre, steps)
                new[z, x] = value + spread(hold, z, x, pad) * total

        return work

    def starter(new, right, gain, index=None):
        pad = size_of(new)[0]

        def work(z, xs):
            for x in xs:
                value = right[z, x] if index is None else pick(right[z, x], index)
                new[z, x] = spread(gain, z, x, pad) * value

        return work

    def defecter(new, old, right, stretch, steps, paired):
        def work(z, xs):
            for x, centre, total in around(old, z, xs, 1.0):
                value = spread(cond, z - PAD + NEAR, x, PAD)
                if stretch != 1.0:
                    value = stretch * value
                left = (right[z, x] + prior(centre, steps)) - centre
                left = left - value * (2.0 * sum(FINE) * centre - total)
                if paired:
                    left = pick(left, evens) + pick(left, evens + 1)
                new[z, x] = left

        return work

    half = peers // 2
    of_half, of_quarter = time % half, time % (half // 2)
    evens = 2 * of_half

    def wide(ref, into, depth, corner, stage, steps):
        pad, deep, broad = size_of(ref)

        def spans(step, size, count):
            if step == 0:
                return pl.ds(pad, size), pl.ds(pad, size)
            if step > 0:
                return pl.ds(pad + size - count, count), pl.ds(pad - count, count)
            return pl.ds(pad, count), pl.ds(pad + size, count)

        out = []
        corners = [(dz, dx) for dz in (1, -1) for dx in (1, -1)]
        for number, (dz, dx) in enumerate(corners + [(0, 1), (0, -1), (1, 0), (-1, 0)]):
            count = corner if dz and dx else depth
            src_z, dst_z = spans(dz, deep, count)
            src_x, dst_x = spans(dx, broad, count)
            some = () if steps == peers else (pl.ds(0, steps),)
            copy = pltpu.make_async_remote_copy(
                src_ref=ref.at[(src_z, src_x, *some)],
                dst_ref=into.at[(dst_z, dst_x, *some)],
                send_sem=h_send.at[stage, number],
                recv_sem=h_recv.at[stage, number],
                device_id=device(dz, dx),
                device_id_type=MESH,
            )
            sends = both(has_z[dz], has_x[dx])
            arrives = both(has_z[-dz], has_x[-dx])
            out.append((sends, arrives, copy))
        return out

    started = {}

    def send(ref, into, depth, corner, stage, steps):
        started[stage] = wide(ref, into, depth, corner, stage, steps)
        for sends, _, copy in started[stage]:
            pl.when(sends)(copy.start)

    def receive(stage):
        for _, arrives, copy in started[stage]:
            pl.when(arrives)(copy.wait_recv)

    def pieces_of(ref, edge):
        _, deep, broad = size_of(ref)
        return (
            (edge, deep - 2 * edge, edge, broad - 2 * edge),
            (0, edge, 0, broad),
            (deep - edge, edge, 0, broad),
            (edge, deep - 2 * edge, 0, edge),
            (edge, deep - 2 * edge, broad - edge, edge),
        )

    pieces = [(a5, out_solution, part) for part in pieces_of(a5, 2)]
    pieces.append((fd, out_defect, (0, planes, 0, block)))

    def ends(piece, step, owner):
        src, dst, (z, deep, x, broad) = pieces[piece]
        return (
            src.at[pl.ds(z + PAD, deep), pl.ds(x + PAD, broad), step, :],
            dst.at[pl.ds(z, deep), pl.ds(snake(owner) * block + x, broad), :],
        )

    def outward(piece, peer, owner):
        src, dst = ends(piece, peer, owner)
        return pltpu.make_async_remote_copy(
            src_ref=src,
            dst_ref=dst,
            send_sem=out_send.at[piece, peer],
            recv_sem=out_recv.at[piece, owner],
            device_id={"tm": peer},
            device_id_type=MESH,
        )

    def home(piece):
        src, dst = ends(piece, me, me)
        return pltpu.make_async_copy(src, dst, out_own.at[piece])

    def ship(piece):
        for k in order:
            outward(piece, me ^ k, me).start()
        home(piece).start()

    own.wait()
    for k in order:
        inward(me, me ^ k, me ^ k).wait_recv()

    send(rhs, rhs, 2, 1, 0, peers)
    first = starter(a1, rhs, gain0)
    second = sweeper(a2, a1, None, gain0, hold0, peers)
    third = defecter(rhs1, a2, rhs, 1.0, peers, True)
    over(a1, 0, None, first)
    over(a2, -1, None, second)
    over(rhs1, -2, None, third)
    receive(0)
    over(a1, 2, 0, first)
    over(a2, 1, -1, second)
    over(rhs1, 0, -2, third)

    send(rhs1, rhs1, 2, 1, 1, half)
    send(a2, a3, 3, 2, 2, peers)
    first = starter(m1, rhs1, gain1, of_half)
    second = sweeper(m2, m1, None, gain1, hold1, half)
    third = defecter(scrap, m2, rhs1, 2.0, half, False)
    over(m1, 0, None, first)
    over(m2, -1, None, second)
    over(scrap, -2, None, third)
    receive(1)
    over(m1, 2, 0, first)
    over(m2, 1, -1, second)
    over(scrap, 0, -2, third)

    pairs = 2 * of_quarter

    def restrict(z, _):
        for x in range(half_block):
            zz, xx = 2 * z + PAD, 2 * x + PAD
            quad = (scrap[zz, xx] + scrap[zz + 1, xx]) + (
                scrap[zz, xx + 1] + scrap[zz + 1, xx + 1]
            )
            rhs2[z + PAD2, x + PAD2] = 0.25 * (pick(quad, pairs) + pick(quad, pairs + 1))
        return 0

    lax.fori_loop(0, half_planes, restrict, 0)
    send(rhs2, rhs2, 4, 4, 3, half // 2)
    send(m2, m3, 2, 1, 4, half)
    start = starter(k1, rhs2, gain2, of_quarter)
    second, third, fourth = (
        sweeper(new, old, first, gain2, hold2, half // 2, 4.0)
        for new, old, first in ((k2, k1, None), (k3, k2, k1), (k4, k3, k1))
    )
    over(k1, 0, None, start)
    over(k2, -1, None, second)
    receive(3)
    over(k1, 4, 0, start)
    over(k2, 3, -1, second)
    over(k3, 2, None, third)
    over(k4, 1, None, fourth)

    halved = of_half // 2

    def prolonger(received):
        def work(z, xs):
            for x in xs:
                value = pick(k4[z, x], halved)
                for dz in range(2):
                    for dx in range(2):
                        at = (2 * (z - PAD2) + dz + PAD, 2 * (x - PAD2) + dx + PAD)
                        base = pick(m3[at], of_half) if received else m2[at]
                        m3[at] = base + value

        return work

    over(k4, 0, None, prolonger(False))
    receive(4)
    over(k4, 1, 0, prolonger(True))
    over(m4, 1, None, sweeper(m4, m3, m1, gain1, hold1, half))
    over(m5, 0, None, sweeper(m5, m4, m1, gain1, hold1, half))
    send(m5, m5, 3, 2, 5, half)

    def joiner(base):
        def work(z, xs):
            for x in xs:
                a3[z, x] = base[z, x] + pick(m5[z, x], time // 2)

        return work

    fourth = sweeper(a4, a3, a1, gain0, hold0, peers)
    fifth = sweeper(a5, a4, a1, gain0, hold0, peers)
    last = defecter(fd, a5, rhs, 1.0, peers, False)
    over(a3, 0, None, joiner(a2))
    over(a4, -1, None, fourth)
    over(a5, -2, None, fifth)
    ship(0)
    over(fd, -3, None, last)
    receive(2)
    receive(5)
    over(a3, 3, 0, joiner(a3))
    over(a4, 2, -1, fourth)
    over(a5, 1, -2, fifth)
    for piece in range(1, 5):
        ship(piece)
    over(fd, 0, -3, last)
    ship(5)

    for copies in started.values():
        for sends, _, copy in copies:
            pl.when(sends)(copy.wait_send)
    for side, dz in ((0, 1), (1, -1)):
        pl.when(has_z[dz])(cond_copy(side, dz).wait_send)
    for k in order:
        inward(me ^ k, me, me).wait_send()
    for piece in range(6):
        home(piece).wait()
        for k in order:
            outward(piece, me ^ k, me).wait_send()
            outward(piece, me, me ^ k).wait_recv()


def fused_body(peers, slabs, source, conductivity):
    _, planes, rows, lanes = source.shape
    block = rows // peers

    def field(depth, width):
        return pltpu.VMEM((depth, width, peers, lanes), jnp.float32)

    def table(depth, width):
        return pltpu.VMEM((depth, width, lanes), jnp.float32)

    large = field(planes + 2 * PAD, block + 2 * PAD)
    small = field(planes // 2 + 2 * PAD2, block // 2 + 2 * PAD2)
    fine = table(planes + 2 * PAD, block + 2 * NEAR)
    coarse = table(planes // 2 + 2 * PAD2, block // 2 + 2 * PAD2)
    dma = pltpu.SemaphoreType.DMA
    anywhere = pl.BlockSpec(memory_space=pl.ANY)
    shape = pltpu.VMEM((planes, rows, lanes), jnp.float32)
    solution, final_defect = pl.pallas_call(
        functools.partial(cycle_kernel, peers, slabs),
        out_shape=(shape, shape),
        in_specs=[anywhere, anywhere],
        out_specs=(anywhere, anywhere),
        scratch_shapes=[
            large, large, small, large,
            table(planes + 2 * NEAR, block + 2 * NEAR),
            fine, fine, fine, fine, coarse, coarse,
            large, large, large, large, large, large,
            large, large, large, large, large,
            small, small, small, small,
            pltpu.VMEM((planes, rows, lanes), jnp.float32),
            dma((peers,)), dma((peers,)), dma, dma, dma((3,)),
            dma((2,)), dma((2,)),
            dma((6, 8)), dma((6, 8)),
            dma((6, peers)), dma((6, peers)), dma((6,)),
        ],
        compiler_params=pltpu.CompilerParams(
            collective_id=0, has_side_effects=True, vmem_limit_bytes=56 * 1024 * 1024
        ),
    )(source[0], conductivity)
    return (solution[None], final_defect[None])


def solution(mesh):
    peers, slabs = mesh.shape["tm"], mesh.shape["space"]

    def chosen(source, conductivity):
        steps, planes, rows, lanes = source.shape
        if fits(steps * peers, peers, slabs, planes, rows, lanes):
            return fused_body(peers, slabs, source, conductivity)
        return body(source, conductivity)

    return jax.shard_map(
        chosen,
        mesh=mesh,
        in_specs=(P("tm", "space", None, None), P("space", None, None)),
        out_specs=(P("tm", "space", None, None), P("tm", "space", None, None)),
        check_vma=False,
    )
```

```python
import functools

import jax
import jax.numpy as jnp
from jax import lax
from jax.experimental import pallas as pl
from jax.experimental.pallas import tpu as pltpu
from jax.sharding import PartitionSpec as P

NU = 2
NC = 4


OMEGA = 0.8
FINE = (1.0, 1.0, 1.0)
COARSE = (0.25, 0.25, 1.0)


def padded_2(shard, sides, width):
    for axis, dim in sides:
        peers, length = (lax.axis_size(axis), shard.shape[dim])
        up = [(i, (i + 1) % peers) for i in range(peers - 1)]
        down = [(j, i) for i, j in up]
        last = lax.slice_in_dim(shard, length - width, length, axis=dim)
        first = lax.slice_in_dim(shard, 0, width, axis=dim)
        before = lax.ppermute(last, axis, up)
        after = lax.ppermute(first, axis, down)
        shard = jnp.concatenate([before, shard, after], axis=dim)
    return shard


def shifted(shard, axis, by):
    peers = lax.axis_size(axis)
    pairs = [(i, i + by) for i in range(peers) if 0 <= i + by < peers]
    return lax.ppermute(shard, axis, pairs)


def swapped(value, axis, bit):
    mask = 2**bit
    pairs = [(source, source ^ mask) for source in range(lax.axis_size(axis))]
    return lax.ppermute(value, axis, pairs)


def stencil(padded, weights):
    weight_z, weight_x, weight_y = weights
    centre = padded[1:-1, :, 1:-1]
    widened = jnp.pad(padded[1:-1], ((0, 0), (1, 1), (0, 0)))
    along_z = 2.0 * centre - padded[2:, :, 1:-1] - padded[:-2, :, 1:-1]
    along_x = 2.0 * centre - widened[:, 2:, 1:-1] - widened[:, :-2, 1:-1]
    along_y = 2.0 * centre - padded[1:-1, :, 2:] - padded[1:-1, :, :-2]
    return weight_z * along_z + weight_x * along_x + weight_y * along_y


def defect(current, right_side, earlier, padded, conduct, stretch, weights):
    applied = current + stretch * conduct * stencil(padded, weights)
    return right_side + earlier - applied


def relaxed(current, right_side, earlier, padded, conduct, stretch, weights):
    weight_sum = 2.0 * (weights[0] + weights[1] + weights[2])
    diagonal = 1.0 + stretch * conduct * weight_sum
    return (
        current
        + OMEGA * defect(current, right_side, earlier, padded, conduct, stretch, weights) / diagonal
    )


def coarsen(values):
    return 0.25 * (
        values[..., 0::2, 0::2, :]
        + values[..., 1::2, 0::2, :]
        + (values[..., 0::2, 1::2, :] + values[..., 1::2, 1::2, :])
    )


def refine(values):
    return jnp.repeat(jnp.repeat(values, 2, axis=-3), 2, axis=-2)


def zero_columns(values):
    return jnp.pad(values, ((0, 0), (0, 0), (1, 1)))


def plane_faces(values):
    return padded_2(values, (("space", 0),), 1)


def coarse_planes_framed(values):
    return padded_2(values, (("space", 0),), 1)


def fine_frame(values):
    return zero_columns(plane_faces(values))


def step_prior(values):
    return shifted(values, "tm", 1)


def pair_prior(values):
    return shifted(values, "tm", 2)


def group_prior(values):
    return shifted(values, "tm", 4)


def smooth(current, right_side, conduct, stretch, weights, repeats, earlier_of, framing):
    for turn_index in range(repeats):
        current = relaxed(
            current, right_side, earlier_of(current), framing(current), conduct, stretch, weights
        )
    return current


def body(source, conductivity):
    right_side = source[0]
    solution = smooth(
        jnp.zeros_like(right_side), right_side, conductivity, 1.0, FINE, NU, step_prior, fine_frame
    )
    defect_fine = defect(
        solution, right_side, step_prior(solution), fine_frame(solution), conductivity, 1.0, FINE
    )
    middle_full = defect_fine + swapped(defect_fine, "tm", 0)
    middle = smooth(
        jnp.zeros_like(middle_full),
        middle_full,
        conductivity,
        2.0,
        FINE,
        NU,
        pair_prior,
        fine_frame,
    )
    middle_defect = defect(
        middle, middle_full, pair_prior(middle), fine_frame(middle), conductivity, 2.0, FINE
    )
    summed = middle_defect + swapped(middle_defect, "tm", 1)
    coarse_rhs = coarsen(summed)
    coarse_cond = coarsen(conductivity)

    def coarse_frame(values):
        return zero_columns(coarse_planes_framed(values))

    coarse = smooth(
        jnp.zeros_like(coarse_rhs),
        coarse_rhs,
        coarse_cond,
        4.0,
        COARSE,
        NC,
        group_prior,
        coarse_frame,
    )
    middle = middle + refine(coarse)
    middle = smooth(middle, middle_full, conductivity, 2.0, FINE, NU, pair_prior, fine_frame)
    solution = solution + middle
    solution = smooth(solution, right_side, conductivity, 1.0, FINE, NU, step_prior, fine_frame)
    final_defect = defect(
        solution, right_side, step_prior(solution), fine_frame(solution), conductivity, 1.0, FINE
    )
    return (solution[None], final_defect[None])


MESH = pl.DeviceIdType.MESH


def snake(index):
    return index + ((index // 2) % 2) * (1 - 2 * (index % 2))


def scaled(weights, stretch):
    return tuple(stretch * weight for weight in weights)


def fits(steps, peers, slabs, planes, rows, lanes):
    block = rows // peers
    return (
        steps == peers
        and peers % 8 == 0
        and peers & (peers - 1) == 0
        and rows % peers == 0
        and block % 8 == 0
        and planes % 2 == 0
        and planes >= 8
        and lanes % 128 == 0
        and peers == 8
        and slabs > 1
    )


PAD, PAD2 = 3, 4
NEAR = 2 * PAD2
UNROLL = 96


def cycle_kernel(
    peers,
    slabs,
    source_far,
    conduct_far,
    out_solution,
    out_defect,
    rhs, rhs1, rhs2, scrap,
    cond, gain0, hold0, gain1, hold1, gain2, hold2,
    a1, a2, a3, a4, a5, fd,
    m1, m2, m3, m4, m5,
    k1, k2, k3, k4,
    source,
    in_send, in_recv, own_sem, load_sem, cond_load,
    cond_send, cond_recv,
    h_send, h_recv,
    out_send, out_recv, out_own,
):
    planes, rows, lanes = source.shape
    block = rows // peers
    half_planes, half_block = planes // 2, block // 2
    me, slab = lax.axis_index("tm"), lax.axis_index("space")
    mine = snake(me)
    following, preceding = snake((mine + 1) % peers), snake((mine + peers - 1) % peers)
    has_z = {1: slab < slabs - 1, -1: slab > 0, 0: None}
    has_x = {1: mine < peers - 1, -1: mine > 0, 0: None}
    beside = {1: following, -1: preceding}

    def both(first, second):
        if first is None:
            return second
        return first if second is None else first & second

    def device(dz, dx):
        where = {}
        if dx:
            where["tm"] = beside[dx]
        if dz:
            where["space"] = slab + dz
        return where

    def size_of(ref):
        pad = PAD2 if ref.shape[0] == half_planes + 2 * PAD2 else PAD
        return pad, ref.shape[0] - 2 * pad, ref.shape[1] - 2 * pad

    def over(ref, outer, inner, work):
        pad, depth, width = size_of(ref)
        z0, z1, x0, x1 = pad - outer, pad + depth + outer, pad - outer, pad + width + outer
        parts = []
        if inner is None:
            parts.append((z0, z1, list(range(x0, x1))))
        else:
            i0, i1, j0, j1 = pad - inner, pad + depth + inner, pad - inner, pad + width + inner
            parts.append((z0, i0, list(range(x0, x1))))
            parts.append((i1, z1, list(range(x0, x1))))
            parts.append((i0, i1, list(range(x0, j0)) + list(range(j1, x1))))
        for first, last, xs in parts:
            count = last - first
            if count <= 0 or not xs:
                continue
            folds = [u for u in range(1, count + 1) if count % u == 0 and u * len(xs) <= UNROLL]
            fold = max(folds) if folds else 1
            if fold == count:
                for z in range(first, last):
                    work(z, xs)
                continue

            def step(i, _, first=first, xs=xs, fold=fold):
                for u in range(fold):
                    work(first + i * fold + u, xs)
                return 0

            lax.fori_loop(0, count // fold, step, 0)

    load_source = pltpu.make_async_copy(source_far, source, load_sem)
    load_source.start()

    def window(number):
        start, count, at = ((0, block, NEAR), (-NEAR, NEAR, 0), (block, NEAR, NEAR + block))[number]
        return pltpu.make_async_copy(
            conduct_far.at[:, pl.ds(pl.multiple_of(mine * block + start, 8), count), :],
            cond.at[pl.ds(NEAR, planes), pl.ds(at, count), :],
            cond_load.at[number],
        )

    window(0).start()
    pl.when(has_x[-1])(window(1).start)
    pl.when(has_x[1])(window(2).start)

    barrier = pltpu.get_barrier_semaphore()
    for k in range(1, peers):
        pl.semaphore_signal(barrier, inc=1, device_id={"tm": me ^ k}, device_id_type=MESH)
    expected = peers - 1
    for dz in (1, -1):
        for dx in (0, 1, -1):
            here = both(has_z[dz], has_x[dx])

            @pl.when(here)
            def _(dz=dz, dx=dx):
                pl.semaphore_signal(
                    barrier, inc=1, device_id=device(dz, dx), device_id_type=MESH
                )

            expected = expected + jnp.where(here, 1, 0)
    load_source.wait()
    pl.semaphore_wait(barrier, expected)

    def rows_of(index):
        return pl.ds(pl.multiple_of(snake(index) * block, 8), block)

    def inward(peer, step, recv):
        return pltpu.make_async_remote_copy(
            src_ref=source.at[:, rows_of(peer), :],
            dst_ref=rhs.at[pl.ds(PAD, planes), pl.ds(PAD, block), step, :],
            send_sem=in_send.at[peer],
            recv_sem=in_recv.at[recv],
            device_id={"tm": peer},
            device_id_type=MESH,
        )

    order = sorted(range(1, peers), reverse=True)
    for k in order:
        inward(me ^ k, me, me).start()
    own = pltpu.make_async_copy(
        source_far.at[:, rows_of(me), :],
        rhs.at[pl.ds(PAD, planes), pl.ds(PAD, block), me, :],
        own_sem,
    )
    own.start()
    window(0).wait()
    pl.when(has_x[-1])(window(1).wait)
    pl.when(has_x[1])(window(2).wait)

    def cond_copy(side, dz):
        return pltpu.make_async_remote_copy(
            src_ref=cond.at[pl.ds(planes, NEAR) if dz > 0 else pl.ds(NEAR, NEAR)],
            dst_ref=cond.at[pl.ds(0, NEAR) if dz > 0 else pl.ds(NEAR + planes, NEAR)],
            send_sem=cond_send.at[side],
            recv_sem=cond_recv.at[side],
            device_id={"space": slab + dz},
            device_id_type=MESH,
        )

    for side, dz in ((0, 1), (1, -1)):
        pl.when(has_z[dz])(cond_copy(side, dz).start)

    for ref in (rhs, rhs1, a3, m3, m5, rhs2):
        pad, deep, broad = size_of(ref)
        for dz, first in ((-1, 0), (1, pad + deep)):

            @pl.when(jnp.logical_not(has_z[dz]))
            def _(ref=ref, first=first, pad=pad):
                def clear(z, _):
                    ref[z] = jnp.zeros(ref.shape[1:], jnp.float32)
                    return 0

                lax.fori_loop(first, first + pad, clear, 0)

        for dx, first in ((-1, 0), (1, pad + broad)):

            @pl.when(jnp.logical_not(has_x[dx]))
            def _(ref=ref, first=first, pad=pad):
                def clear(z, _):
                    ref[z, first : first + pad] = jnp.zeros((pad, peers, lanes), jnp.float32)
                    return 0

                lax.fori_loop(0, ref.shape[0], clear, 0)

    for side, dz in ((0, 1), (1, -1)):
        pl.when(has_z[-dz])(cond_copy(side, dz).wait_recv)

    def fill(z, _):
        plane = slab * planes + z - PAD
        deep = (plane >= 0) & (plane < slabs * planes)
        for part in range((block + 2 * NEAR) // 8):
            at = pl.ds(8 * part, 8)
            row = mine * block - NEAR + 8 * part + lax.broadcasted_iota(jnp.int32, (8, lanes), 0)
            ok = deep & (row >= 0) & (row < rows)
            value = jnp.where(ok, cond[z - PAD + NEAR, at, :], 0.0)
            fine = jnp.where(ok, OMEGA / (1.0 + value * (2.0 * sum(FINE))), 0.0)
            middle = jnp.where(ok, OMEGA / (1.0 + value * (4.0 * sum(FINE))), 0.0)
            gain0[z, at, :] = fine
            hold0[z, at, :] = fine * value
            gain1[z, at, :] = middle
            hold1[z, at, :] = middle * (2.0 * value)
        return 0

    lax.fori_loop(0, planes + 2 * PAD, fill, 0)

    def fill2(z, _):
        plane = slab * half_planes + z - PAD2
        deep = (plane >= 0) & (plane < slabs * half_planes)
        for part in range((block + 2 * NEAR) // 16):
            at = pl.ds(8 * part, 8)
            even, odd = pl.ds(16 * part, 8, stride=2), pl.ds(16 * part + 1, 8, stride=2)
            quad = (cond[2 * z, even, :] + cond[2 * z + 1, even, :]) + (
                cond[2 * z, odd, :] + cond[2 * z + 1, odd, :]
            )
            row = mine * half_block - PAD2 + 8 * part
            row = row + lax.broadcasted_iota(jnp.int32, (8, lanes), 0)
            ok = deep & (row >= 0) & (row < rows // 2)
            value = jnp.where(ok, 0.25 * quad, 0.0)
            gain = jnp.where(ok, OMEGA / (1.0 + value * (8.0 * sum(COARSE))), 0.0)
            gain2[z, at, :] = gain
            hold2[z, at, :] = gain * value
        return 0

    lax.fori_loop(0, half_planes + 2 * PAD2, fill2, 0)

    time = lax.broadcasted_iota(jnp.int32, (peers, lanes), 0)
    lane = lax.broadcasted_iota(jnp.int32, (peers, lanes), 1)
    not_first, not_last = lane > 0, lane < lanes - 1
    later = {count: time % count > 0 for count in (peers, peers // 2, peers // 4)}

    def pick(value, index):
        return jnp.take_along_axis(value, index, axis=0, mode="promise_in_bounds")

    def prior(value, steps):
        return jnp.where(later[steps], pltpu.roll(value, 1, 0), 0.0)

    def spread(ref, z, x, pad):
        near = PAD2 if pad == PAD2 else NEAR
        return jnp.broadcast_to(ref[z, pl.ds(x - pad + near, 1), :], (peers, lanes))

    def around(ref, z, xs, weight_y):
        wanted = sorted({x + step for x in xs for step in (-1, 0, 1)})
        row = {x: ref[z, x] for x in wanted}
        for x in xs:
            centre = row[x]
            across = (ref[z - 1, x] + ref[z + 1, x]) + (row[x - 1] + row[x + 1])
            along = jnp.where(not_first, pltpu.roll(centre, 1, 1), 0.0) + jnp.where(
                not_last, pltpu.roll(centre, lanes - 1, 1), 0.0
            )
            total = across + along if weight_y == 1.0 else across + weight_y * along
            yield x, centre, total

    def sweeper(new, old, first, gain, hold, steps, weight_y=1.0):
        pad = size_of(new)[0]

        def work(z, xs):
            for x, centre, total in around(old, z, xs, weight_y):
                if first is None:
                    value = (2.0 - OMEGA) * centre
                else:
                    value = (1.0 - OMEGA) * centre + first[z, x]
                value = value + spread(gain, z, x, pad) * prior(centre, steps)
                new[z, x] = value + spread(hold, z, x, pad) * total

        return work

    def starter(new, right, gain, index=None):
        pad = size_of(new)[0]

        def work(z, xs):
            for x in xs:
                value = right[z, x] if index is None else pick(right[z, x], index)
                new[z, x] = spread(gain, z, x, pad) * value

        return work

    def defecter(new, old, right, stretch, steps, paired):
        def work(z, xs):
            for x, centre, total in around(old, z, xs, 1.0):
                value = spread(cond, z - PAD + NEAR, x, PAD)
                if stretch != 1.0:
                    value = stretch * value
                left = (right[z, x] + prior(centre, steps)) - centre
                left = left - value * (2.0 * sum(FINE) * centre - total)
                if paired:
                    left = pick(left, evens) + pick(left, evens + 1)
                new[z, x] = left

        return work

    half = peers // 2
    of_half, of_quarter = time % half, time % (half // 2)
    evens = 2 * of_half

    def wide(ref, into, depth, corner, stage, steps):
        pad, deep, broad = size_of(ref)

        def spans(step, size, count):
            if step == 0:
                return pl.ds(pad, size), pl.ds(pad, size)
            if step > 0:
                return pl.ds(pad + size - count, count), pl.ds(pad - count, count)
            return pl.ds(pad, count), pl.ds(pad + size, count)

        out = []
        corners = [(dz, dx) for dz in (1, -1) for dx in (1, -1)]
        for number, (dz, dx) in enumerate(corners + [(0, 1), (0, -1), (1, 0), (-1, 0)]):
            count = corner if dz and dx else depth
            src_z, dst_z = spans(dz, deep, count)
            src_x, dst_x = spans(dx, broad, count)
            some = () if steps == peers else (pl.ds(0, steps),)
            copy = pltpu.make_async_remote_copy(
                src_ref=ref.at[(src_z, src_x, *some)],
                dst_ref=into.at[(dst_z, dst_x, *some)],
                send_sem=h_send.at[stage, number],
                recv_sem=h_recv.at[stage, number],
                device_id=device(dz, dx),
                device_id_type=MESH,
            )
            sends = both(has_z[dz], has_x[dx])
            arrives = both(has_z[-dz], has_x[-dx])
            out.append((sends, arrives, copy))
        return out

    started = {}

    def send(ref, into, depth, corner, stage, steps):
        started[stage] = wide(ref, into, depth, corner, stage, steps)
        for sends, _, copy in started[stage]:
            pl.when(sends)(copy.start)

    def receive(stage):
        for _, arrives, copy in started[stage]:
            pl.when(arrives)(copy.wait_recv)

    def pieces_of(ref, edge):
        _, deep, broad = size_of(ref)
        return (
            (edge, deep - 2 * edge, edge, broad - 2 * edge),
            (0, edge, 0, broad),
            (deep - edge, edge, 0, broad),
            (edge, deep - 2 * edge, 0, edge),
            (edge, deep - 2 * edge, broad - edge, edge),
        )

    pieces = [(a5, out_solution, part) for part in pieces_of(a5, 2)]
    pieces.append((fd, out_defect, (0, planes, 0, block)))

    def ends(piece, step, owner):
        src, dst, (z, deep, x, broad) = pieces[piece]
        return (
            src.at[pl.ds(z + PAD, deep), pl.ds(x + PAD, broad), step, :],
            dst.at[pl.ds(z, deep), pl.ds(snake(owner) * block + x, broad), :],
        )

    def outward(piece, peer, owner):
        src, dst = ends(piece, peer, owner)
        return pltpu.make_async_remote_copy(
            src_ref=src,
            dst_ref=dst,
            send_sem=out_send.at[piece, peer],
            recv_sem=out_recv.at[piece, owner],
            device_id={"tm": peer},
            device_id_type=MESH,
        )

    def home(piece):
        src, dst = ends(piece, me, me)
        return pltpu.make_async_copy(src, dst, out_own.at[piece])

    def ship(piece):
        for k in order:
            outward(piece, me ^ k, me).start()
        home(piece).start()

    own.wait()
    for k in order:
        inward(me, me ^ k, me ^ k).wait_recv()

    send(rhs, rhs, 2, 1, 0, peers)
    first = starter(a1, rhs, gain0)
    second = sweeper(a2, a1, None, gain0, hold0, peers)
    third = defecter(rhs1, a2, rhs, 1.0, peers, True)
    over(a1, 0, None, first)
    over(a2, -1, None, second)
    over(rhs1, -2, None, third)
    receive(0)
    over(a1, 2, 0, first)
    over(a2, 1, -1, second)
    over(rhs1, 0, -2, third)

    send(rhs1, rhs1, 2, 1, 1, half)
    send(a2, a3, 3, 2, 2, peers)
    first = starter(m1, rhs1, gain1, of_half)
    second = sweeper(m2, m1, None, gain1, hold1, half)
    third = defecter(scrap, m2, rhs1, 2.0, half, False)
    over(m1, 0, None, first)
    over(m2, -1, None, second)
    over(scrap, -2, None, third)
    receive(1)
    over(m1, 2, 0, first)
    over(m2, 1, -1, second)
    over(scrap, 0, -2, third)

    pairs = 2 * of_quarter

    def restrict(z, _):
        for x in range(half_block):
            zz, xx = 2 * z + PAD, 2 * x + PAD
            quad = (scrap[zz, xx] + scrap[zz + 1, xx]) + (
                scrap[zz, xx + 1] + scrap[zz + 1, xx + 1]
            )
            rhs2[z + PAD2, x + PAD2] = 0.25 * (pick(quad, pairs) + pick(quad, pairs + 1))
        return 0

    lax.fori_loop(0, half_planes, restrict, 0)
    send(rhs2, rhs2, 4, 4, 3, half // 2)
    send(m2, m3, 2, 1, 4, half)
    start = starter(k1, rhs2, gain2, of_quarter)
    second, third, fourth = (
        sweeper(new, old, first, gain2, hold2, half // 2, 4.0)
        for new, old, first in ((k2, k1, None), (k3, k2, k1), (k4, k3, k1))
    )
    over(k1, 0, None, start)
    over(k2, -1, None, second)
    receive(3)
    over(k1, 4, 0, start)
    over(k2, 3, -1, second)
    over(k3, 2, None, third)
    over(k4, 1, None, fourth)

    halved = of_half // 2

    def prolonger(received):
        def work(z, xs):
            for x in xs:
                value = pick(k4[z, x], halved)
                for dz in range(2):
                    for dx in range(2):
                        at = (2 * (z - PAD2) + dz + PAD, 2 * (x - PAD2) + dx + PAD)
                        base = pick(m3[at], of_half) if received else m2[at]
                        m3[at] = base + value

        return work

    over(k4, 0, None, prolonger(False))
    receive(4)
    over(k4, 1, 0, prolonger(True))
    over(m4, 1, None, sweeper(m4, m3, m1, gain1, hold1, half))
    over(m5, 0, None, sweeper(m5, m4, m1, gain1, hold1, half))
    send(m5, m5, 3, 2, 5, half)

    def joiner(base):
        def work(z, xs):
            for x in xs:
                a3[z, x] = base[z, x] + pick(m5[z, x], time // 2)

        return work

    fourth = sweeper(a4, a3, a1, gain0, hold0, peers)
    fifth = sweeper(a5, a4, a1, gain0, hold0, peers)
    last = defecter(fd, a5, rhs, 1.0, peers, False)
    over(a3, 0, None, joiner(a2))
    over(a4, -1, None, fourth)
    over(a5, -2, None, fifth)
    ship(0)
    over(fd, -3, None, last)
    receive(2)
    receive(5)
    over(a3, 3, 0, joiner(a3))
    over(a4, 2, -1, fourth)
    over(a5, 1, -2, fifth)
    for piece in range(1, 5):
        ship(piece)
    over(fd, 0, -3, last)
    ship(5)

    for copies in started.values():
        for sends, _, copy in copies:
            pl.when(sends)(copy.wait_send)
    for side, dz in ((0, 1), (1, -1)):
        pl.when(has_z[dz])(cond_copy(side, dz).wait_send)
    for k in order:
        inward(me ^ k, me, me).wait_send()
    for piece in range(6):
        home(piece).wait()
        for k in order:
            outward(piece, me ^ k, me).wait_send()
            outward(piece, me, me ^ k).wait_recv()


def fused_body(peers, slabs, source, conductivity):
    _, planes, rows, lanes = source.shape
    block = rows // peers

    def field(depth, width):
        return pltpu.VMEM((depth, width, peers, lanes), jnp.float32)

    def table(depth, width):
        return pltpu.VMEM((depth, width, lanes), jnp.float32)

    large = field(planes + 2 * PAD, block + 2 * PAD)
    small = field(planes // 2 + 2 * PAD2, block // 2 + 2 * PAD2)
    fine = table(planes + 2 * PAD, block + 2 * NEAR)
    coarse = table(planes // 2 + 2 * PAD2, block // 2 + 2 * PAD2)
    dma = pltpu.SemaphoreType.DMA
    anywhere = pl.BlockSpec(memory_space=pl.ANY)
    shape = pltpu.VMEM((planes, rows, lanes), jnp.float32)
    solution, final_defect = pl.pallas_call(
        functools.partial(cycle_kernel, peers, slabs),
        out_shape=(shape, shape),
        in_specs=[anywhere, anywhere],
        out_specs=(anywhere, anywhere),
        scratch_shapes=[
            large, large, small, large,
            table(planes + 2 * NEAR, block + 2 * NEAR),
            fine, fine, fine, fine, coarse, coarse,
            large, large, large, large, large, large,
            large, large, large, large, large,
            small, small, small, small,
            pltpu.VMEM((planes, rows, lanes), jnp.float32),
            dma((peers,)), dma((peers,)), dma, dma, dma((3,)),
            dma((2,)), dma((2,)),
            dma((6, 8)), dma((6, 8)),
            dma((6, peers)), dma((6, peers)), dma((6,)),
        ],
        compiler_params=pltpu.CompilerParams(
            collective_id=0, has_side_effects=True, vmem_limit_bytes=56 * 1024 * 1024
        ),
    )(source[0], conductivity)
    return (solution[None], final_defect[None])


def solution(mesh):
    peers, slabs = mesh.shape["tm"], mesh.shape["space"]

    def chosen(source, conductivity):
        steps, planes, rows, lanes = source.shape
        if fits(steps * peers, peers, slabs, planes, rows, lanes):
            return fused_body(peers, slabs, source, conductivity)
        return body(source, conductivity)

    return jax.shard_map(
        chosen,
        mesh=mesh,
        in_specs=(P("tm", "space", None, None), P("space", None, None)),
        out_specs=(P("tm", "space", None, None), P("tm", "space", None, None)),
        check_vma=False,
    )
```

```python
import functools

import jax
import jax.numpy as jnp
from jax import lax
from jax.experimental import pallas as pl
from jax.experimental.pallas import tpu as pltpu
from jax.sharding import PartitionSpec as P

NU = 2
NC = 4


OMEGA = 0.8
FINE = (1.0, 1.0, 1.0)
COARSE = (0.25, 0.25, 1.0)


def padded_2(shard, sides, width):
    for axis, dim in sides:
        peers, length = (lax.axis_size(axis), shard.shape[dim])
        up = [(i, (i + 1) % peers) for i in range(peers - 1)]
        down = [(j, i) for i, j in up]
        last = lax.slice_in_dim(shard, length - width, length, axis=dim)
        first = lax.slice_in_dim(shard, 0, width, axis=dim)
        before = lax.ppermute(last, axis, up)
        after = lax.ppermute(first, axis, down)
        shard = jnp.concatenate([before, shard, after], axis=dim)
    return shard


def shifted(shard, axis, by):
    peers = lax.axis_size(axis)
    pairs = [(i, i + by) for i in range(peers) if 0 <= i + by < peers]
    return lax.ppermute(shard, axis, pairs)


def swapped(value, axis, bit):
    mask = 2**bit
    pairs = [(source, source ^ mask) for source in range(lax.axis_size(axis))]
    return lax.ppermute(value, axis, pairs)


def stencil(padded, weights):
    weight_z, weight_x, weight_y = weights
    centre = padded[1:-1, :, 1:-1]
    widened = jnp.pad(padded[1:-1], ((0, 0), (1, 1), (0, 0)))
    along_z = 2.0 * centre - padded[2:, :, 1:-1] - padded[:-2, :, 1:-1]
    along_x = 2.0 * centre - widened[:, 2:, 1:-1] - widened[:, :-2, 1:-1]
    along_y = 2.0 * centre - padded[1:-1, :, 2:] - padded[1:-1, :, :-2]
    return weight_z * along_z + weight_x * along_x + weight_y * along_y


def defect(current, right_side, earlier, padded, conduct, stretch, weights):
    applied = current + stretch * conduct * stencil(padded, weights)
    return right_side + earlier - applied


def relaxed(current, right_side, earlier, padded, conduct, stretch, weights):
    weight_sum = 2.0 * (weights[0] + weights[1] + weights[2])
    diagonal = 1.0 + stretch * conduct * weight_sum
    return (
        current
        + OMEGA * defect(current, right_side, earlier, padded, conduct, stretch, weights) / diagonal
    )


def coarsen(values):
    return 0.25 * (
        values[..., 0::2, 0::2, :]
        + values[..., 1::2, 0::2, :]
        + (values[..., 0::2, 1::2, :] + values[..., 1::2, 1::2, :])
    )


def refine(values):
    return jnp.repeat(jnp.repeat(values, 2, axis=-3), 2, axis=-2)


def zero_columns(values):
    return jnp.pad(values, ((0, 0), (0, 0), (1, 1)))


def plane_faces(values):
    return padded_2(values, (("space", 0),), 1)


def coarse_planes_framed(values):
    return padded_2(values, (("space", 0),), 1)


def fine_frame(values):
    return zero_columns(plane_faces(values))


def step_prior(values):
    return shifted(values, "tm", 1)


def pair_prior(values):
    return shifted(values, "tm", 2)


def group_prior(values):
    return shifted(values, "tm", 4)


def smooth(current, right_side, conduct, stretch, weights, repeats, earlier_of, framing):
    for turn_index in range(repeats):
        current = relaxed(
            current, right_side, earlier_of(current), framing(current), conduct, stretch, weights
        )
    return current


def body(source, conductivity):
    right_side = source[0]
    solution = smooth(
        jnp.zeros_like(right_side), right_side, conductivity, 1.0, FINE, NU, step_prior, fine_frame
    )
    defect_fine = defect(
        solution, right_side, step_prior(solution), fine_frame(solution), conductivity, 1.0, FINE
    )
    middle_full = defect_fine + swapped(defect_fine, "tm", 0)
    middle = smooth(
        jnp.zeros_like(middle_full),
        middle_full,
        conductivity,
        2.0,
        FINE,
        NU,
        pair_prior,
        fine_frame,
    )
    middle_defect = defect(
        middle, middle_full, pair_prior(middle), fine_frame(middle), conductivity, 2.0, FINE
    )
    summed = middle_defect + swapped(middle_defect, "tm", 1)
    coarse_rhs = coarsen(summed)
    coarse_cond = coarsen(conductivity)

    def coarse_frame(values):
        return zero_columns(coarse_planes_framed(values))

    coarse = smooth(
        jnp.zeros_like(coarse_rhs),
        coarse_rhs,
        coarse_cond,
        4.0,
        COARSE,
        NC,
        group_prior,
        coarse_frame,
    )
    middle = middle + refine(coarse)
    middle = smooth(middle, middle_full, conductivity, 2.0, FINE, NU, pair_prior, fine_frame)
    solution = solution + middle
    solution = smooth(solution, right_side, conductivity, 1.0, FINE, NU, step_prior, fine_frame)
    final_defect = defect(
        solution, right_side, step_prior(solution), fine_frame(solution), conductivity, 1.0, FINE
    )
    return (solution[None], final_defect[None])


MESH = pl.DeviceIdType.MESH


def snake(index):
    return index + ((index // 2) % 2) * (1 - 2 * (index % 2))


def scaled(weights, stretch):
    return tuple(stretch * weight for weight in weights)


def fits(steps, peers, slabs, planes, rows, lanes):
    block = rows // peers
    return (
        steps == peers
        and peers % 8 == 0
        and peers & (peers - 1) == 0
        and rows % peers == 0
        and block % 8 == 0
        and planes % 2 == 0
        and planes >= 8
        and lanes % 128 == 0
        and peers == 8
        and slabs > 1
    )


PAD, PAD2 = 3, 4
NEAR = 2 * PAD2
UNROLL = 96


def cycle_kernel(
    peers,
    slabs,
    source_far,
    conduct_far,
    out_solution,
    out_defect,
    rhs, rhs1, rhs2, scrap,
    cond, gain0, hold0, gain1, hold1, gain2, hold2,
    a1, a2, a3, a4, a5, fd,
    m1, m2, m3, m4, m5,
    k1, k2, k3, k4,
    source, before, outer, conduct,
    in_send, in_recv, own_sem, load_sem, cond_load, conduct_load,
    cond_send, cond_recv,
    h_send, h_recv,
    late_send, early_send, pair_send, relay_send, sol_recv, before_recv,
    sol_own, before_own, fd_send, fd_recv, fd_own, outer_send, outer_recv,
):
    planes, rows, lanes = source.shape
    block = rows // peers
    half_planes, half_block = planes // 2, block // 2
    me, slab = lax.axis_index("tm"), lax.axis_index("space")
    mine = snake(me)
    following, preceding = snake((mine + 1) % peers), snake((mine + peers - 1) % peers)
    has_z = {1: slab < slabs - 1, -1: slab > 0, 0: None}
    has_x = {1: mine < peers - 1, -1: mine > 0, 0: None}
    beside = {1: following, -1: preceding}

    def both(first, second):
        if first is None:
            return second
        return first if second is None else first & second

    def device(dz, dx):
        where = {}
        if dx:
            where["tm"] = beside[dx]
        if dz:
            where["space"] = slab + dz
        return where

    def size_of(ref):
        pad = PAD2 if ref.shape[0] == half_planes + 2 * PAD2 else PAD
        return pad, ref.shape[0] - 2 * pad, ref.shape[1] - 2 * pad

    def over(ref, outer, inner, work):
        pad, depth, width = size_of(ref)
        z0, z1, x0, x1 = pad - outer, pad + depth + outer, pad - outer, pad + width + outer
        parts = []
        if inner is None:
            parts.append((z0, z1, list(range(x0, x1))))
        else:
            i0, i1, j0, j1 = pad - inner, pad + depth + inner, pad - inner, pad + width + inner
            parts.append((z0, i0, list(range(x0, x1))))
            parts.append((i1, z1, list(range(x0, x1))))
            parts.append((i0, i1, list(range(x0, j0)) + list(range(j1, x1))))
        for first, last, xs in parts:
            count = last - first
            if count <= 0 or not xs:
                continue
            folds = [u for u in range(1, count + 1) if count % u == 0 and u * len(xs) <= UNROLL]
            fold = max(folds) if folds else 1
            if fold == count:
                for z in range(first, last):
                    work(z, xs)
                continue

            def step(i, _, first=first, xs=xs, fold=fold):
                for u in range(fold):
                    work(first + i * fold + u, xs)
                return 0

            lax.fori_loop(0, count // fold, step, 0)

    load_source = pltpu.make_async_copy(source_far, source, load_sem)
    load_source.start()

    def window(number):
        start, count, at = ((0, block, NEAR), (-NEAR, NEAR, 0), (block, NEAR, NEAR + block))[number]
        return pltpu.make_async_copy(
            conduct_far.at[:, pl.ds(pl.multiple_of(mine * block + start, 8), count), :],
            cond.at[pl.ds(NEAR, planes), pl.ds(at, count), :],
            cond_load.at[number],
        )

    load_whole = pltpu.make_async_copy(conduct_far, conduct, conduct_load)
    window(0).start()
    pl.when(has_x[-1])(window(1).start)
    pl.when(has_x[1])(window(2).start)

    barrier = pltpu.get_barrier_semaphore()
    for k in range(1, peers):
        pl.semaphore_signal(barrier, inc=1, device_id={"tm": me ^ k}, device_id_type=MESH)
    expected = peers - 1
    for dz in (1, -1):
        for dx in (0, 1, -1):
            here = both(has_z[dz], has_x[dx])

            @pl.when(here)
            def _(dz=dz, dx=dx):
                pl.semaphore_signal(
                    barrier, inc=1, device_id=device(dz, dx), device_id_type=MESH
                )

            expected = expected + jnp.where(here, 1, 0)
    load_source.wait()
    pl.semaphore_wait(barrier, expected)

    def rows_of(index):
        return pl.ds(pl.multiple_of(snake(index) * block, 8), block)

    def inward(peer, step, recv):
        return pltpu.make_async_remote_copy(
            src_ref=source.at[:, rows_of(peer), :],
            dst_ref=rhs.at[pl.ds(PAD, planes), pl.ds(PAD, block), step, :],
            send_sem=in_send.at[peer],
            recv_sem=in_recv.at[recv],
            device_id={"tm": peer},
            device_id_type=MESH,
        )

    order = sorted(range(1, peers), reverse=True)
    for k in order:
        inward(me ^ k, me, me).start()
    own = pltpu.make_async_copy(
        source_far.at[:, rows_of(me), :],
        rhs.at[pl.ds(PAD, planes), pl.ds(PAD, block), me, :],
        own_sem,
    )
    own.start()
    load_whole.start()
    window(0).wait()
    pl.when(has_x[-1])(window(1).wait)
    pl.when(has_x[1])(window(2).wait)

    def cond_copy(side, dz):
        return pltpu.make_async_remote_copy(
            src_ref=cond.at[pl.ds(planes, NEAR) if dz > 0 else pl.ds(NEAR, NEAR)],
            dst_ref=cond.at[pl.ds(0, NEAR) if dz > 0 else pl.ds(NEAR + planes, NEAR)],
            send_sem=cond_send.at[side],
            recv_sem=cond_recv.at[side],
            device_id={"space": slab + dz},
            device_id_type=MESH,
        )

    for side, dz in ((0, 1), (1, -1)):
        pl.when(has_z[dz])(cond_copy(side, dz).start)

    for side, dz in ((0, -1), (1, 1)):

        @pl.when(jnp.logical_not(has_z[dz]))
        def _(side=side):
            outer[side] = jnp.zeros((rows, lanes), jnp.float32)

    for ref in (rhs, rhs1, a3, m3, m5, rhs2):
        pad, deep, broad = size_of(ref)
        for dz, first in ((-1, 0), (1, pad + deep)):

            @pl.when(jnp.logical_not(has_z[dz]))
            def _(ref=ref, first=first, pad=pad):
                def clear(z, _):
                    ref[z] = jnp.zeros(ref.shape[1:], jnp.float32)
                    return 0

                lax.fori_loop(first, first + pad, clear, 0)

        for dx, first in ((-1, 0), (1, pad + broad)):

            @pl.when(jnp.logical_not(has_x[dx]))
            def _(ref=ref, first=first, pad=pad):
                def clear(z, _):
                    ref[z, first : first + pad] = jnp.zeros((pad, peers, lanes), jnp.float32)
                    return 0

                lax.fori_loop(0, ref.shape[0], clear, 0)

    for side, dz in ((0, 1), (1, -1)):
        pl.when(has_z[-dz])(cond_copy(side, dz).wait_recv)

    def fill(z, _):
        plane = slab * planes + z - PAD
        deep = (plane >= 0) & (plane < slabs * planes)
        for part in range((block + 2 * NEAR) // 8):
            at = pl.ds(8 * part, 8)
            row = mine * block - NEAR + 8 * part + lax.broadcasted_iota(jnp.int32, (8, lanes), 0)
            ok = deep & (row >= 0) & (row < rows)
            value = jnp.where(ok, cond[z - PAD + NEAR, at, :], 0.0)
            fine = jnp.where(ok, OMEGA / (1.0 + value * (2.0 * sum(FINE))), 0.0)
            middle = jnp.where(ok, OMEGA / (1.0 + value * (4.0 * sum(FINE))), 0.0)
            gain0[z, at, :] = fine
            hold0[z, at, :] = fine * value
            gain1[z, at, :] = middle
            hold1[z, at, :] = middle * (2.0 * value)
        return 0

    lax.fori_loop(0, planes + 2 * PAD, fill, 0)

    def fill2(z, _):
        plane = slab * half_planes + z - PAD2
        deep = (plane >= 0) & (plane < slabs * half_planes)
        for part in range((block + 2 * NEAR) // 16):
            at = pl.ds(8 * part, 8)
            even, odd = pl.ds(16 * part, 8, stride=2), pl.ds(16 * part + 1, 8, stride=2)
            quad = (cond[2 * z, even, :] + cond[2 * z + 1, even, :]) + (
                cond[2 * z, odd, :] + cond[2 * z + 1, odd, :]
            )
            row = mine * half_block - PAD2 + 8 * part
            row = row + lax.broadcasted_iota(jnp.int32, (8, lanes), 0)
            ok = deep & (row >= 0) & (row < rows // 2)
            value = jnp.where(ok, 0.25 * quad, 0.0)
            gain = jnp.where(ok, OMEGA / (1.0 + value * (8.0 * sum(COARSE))), 0.0)
            gain2[z, at, :] = gain
            hold2[z, at, :] = gain * value
        return 0

    lax.fori_loop(0, half_planes + 2 * PAD2, fill2, 0)

    time = lax.broadcasted_iota(jnp.int32, (peers, lanes), 0)
    lane = lax.broadcasted_iota(jnp.int32, (peers, lanes), 1)
    not_first, not_last = lane > 0, lane < lanes - 1
    later = {count: time % count > 0 for count in (peers, peers // 2, peers // 4)}

    def pick(value, index):
        return jnp.take_along_axis(value, index, axis=0, mode="promise_in_bounds")

    def prior(value, steps):
        return jnp.where(later[steps], pltpu.roll(value, 1, 0), 0.0)

    def spread(ref, z, x, pad):
        near = PAD2 if pad == PAD2 else NEAR
        return jnp.broadcast_to(ref[z, pl.ds(x - pad + near, 1), :], (peers, lanes))

    def around(ref, z, xs, weight_y):
        wanted = sorted({x + step for x in xs for step in (-1, 0, 1)})
        row = {x: ref[z, x] for x in wanted}
        for x in xs:
            centre = row[x]
            across = (ref[z - 1, x] + ref[z + 1, x]) + (row[x - 1] + row[x + 1])
            along = jnp.where(not_first, pltpu.roll(centre, 1, 1), 0.0) + jnp.where(
                not_last, pltpu.roll(centre, lanes - 1, 1), 0.0
            )
            total = across + along if weight_y == 1.0 else across + weight_y * along
            yield x, centre, total

    def sweeper(new, old, first, gain, hold, steps, weight_y=1.0):
        pad = size_of(new)[0]

        def work(z, xs):
            for x, centre, total in around(old, z, xs, weight_y):
                if first is None:
                    value = (2.0 - OMEGA) * centre
                else:
                    value = (1.0 - OMEGA) * centre + first[z, x]
                value = value + spread(gain, z, x, pad) * prior(centre, steps)
                new[z, x] = value + spread(hold, z, x, pad) * total

        return work

    def starter(new, right, gain, index=None):
        pad = size_of(new)[0]

        def work(z, xs):
            for x in xs:
                value = right[z, x] if index is None else pick(right[z, x], index)
                new[z, x] = spread(gain, z, x, pad) * value

        return work

    def defecter(new, old, right, stretch, steps, paired):
        def work(z, xs):
            for x, centre, total in around(old, z, xs, 1.0):
                value = spread(cond, z - PAD + NEAR, x, PAD)
                if stretch != 1.0:
                    value = stretch * value
                left = (right[z, x] + prior(centre, steps)) - centre
                left = left - value * (2.0 * sum(FINE) * centre - total)
                if paired:
                    left = pick(left, evens) + pick(left, evens + 1)
                new[z, x] = left

        return work

    half = peers // 2
    of_half, of_quarter = time % half, time % (half // 2)
    evens = 2 * of_half

    def wide(ref, into, depth, corner, stage, steps):
        pad, deep, broad = size_of(ref)

        def spans(step, size, count):
            if step == 0:
                return pl.ds(pad, size), pl.ds(pad, size)
            if step > 0:
                return pl.ds(pad + size - count, count), pl.ds(pad - count, count)
            return pl.ds(pad, count), pl.ds(pad + size, count)

        out = []
        corners = [(dz, dx) for dz in (1, -1) for dx in (1, -1)]
        for number, (dz, dx) in enumerate(corners + [(0, 1), (0, -1), (1, 0), (-1, 0)]):
            count = corner if dz and dx else depth
            src_z, dst_z = spans(dz, deep, count)
            src_x, dst_x = spans(dx, broad, count)
            some = () if steps == peers else (pl.ds(0, steps),)
            copy = pltpu.make_async_remote_copy(
                src_ref=ref.at[(src_z, src_x, *some)],
                dst_ref=into.at[(dst_z, dst_x, *some)],
                send_sem=h_send.at[stage, number],
                recv_sem=h_recv.at[stage, number],
                device_id=device(dz, dx),
                device_id_type=MESH,
            )
            sends = both(has_z[dz], has_x[dx])
            arrives = both(has_z[-dz], has_x[-dx])
            out.append((sends, arrives, copy))
        return out

    started = {}

    def send(ref, into, depth, corner, stage, steps):
        started[stage] = wide(ref, into, depth, corner, stage, steps)
        for sends, _, copy in started[stage]:
            pl.when(sends)(copy.start)

    def receive(stage):
        for _, arrives, copy in started[stage]:
            pl.when(arrives)(copy.wait_recv)

    def pieces_of(ref, edge):
        _, deep, broad = size_of(ref)
        return (
            (edge, deep - 2 * edge, edge, broad - 2 * edge),
            (0, edge, 0, broad),
            (deep - edge, edge, 0, broad),
            (edge, deep - 2 * edge, 0, edge),
            (edge, deep - 2 * edge, broad - edge, edge),
        )

    parts = pieces_of(a5, 2)
    pair, odd = me // 2, me % 2
    partner = me + 1 - 2 * odd
    others = sorted(range(1, peers // 2), reverse=True)

    def on_parity(work):
        pl.when(odd == 0)(functools.partial(work, 0))
        pl.when(odd == 1)(functools.partial(work, 1))

    def cut(step, piece):
        z, deep, x, broad = parts[piece]
        return a5.at[pl.ds(z + PAD, deep), pl.ds(x + PAD, broad), step, :]

    def laid(ref, owner, piece):
        z, deep, x, broad = parts[piece]
        return ref.at[pl.ds(z, deep), pl.ds(snake(owner) * block + x, broad), :]

    def place(parity):
        return (before, before_recv) if parity else (out_solution, sol_recv)

    def remote(src, dst, send_sem, recv_sem, peer):
        return pltpu.make_async_remote_copy(
            src_ref=src,
            dst_ref=dst,
            send_sem=send_sem,
            recv_sem=recv_sem,
            device_id={"tm": peer},
            device_id_type=MESH,
        )

    def late(piece, group, owner, peer):
        return remote(
            cut(peer, piece), laid(out_solution, owner, piece),
            late_send.at[piece, group], sol_recv.at[piece, owner], peer,
        )

    def early(parity, piece, group, owner, step, peer):
        into, arrived = place(parity)
        return remote(
            cut(step, piece), laid(into, owner, piece),
            early_send.at[piece, group], arrived.at[piece, owner], peer,
        )

    def to_partner(parity, piece, owner):
        into, arrived = place(1 - parity)
        return remote(
            cut(2 * pair, piece), laid(into, owner, piece),
            pair_send.at[piece], arrived.at[piece, owner], partner,
        )

    def relay(parity, piece, group, owner):
        source_of = place(parity)[0]
        into, arrived = place(1 - parity)
        return remote(
            laid(source_of, owner, piece), laid(into, owner, piece),
            relay_send.at[piece, group], arrived.at[piece, owner], partner,
        )

    def own_solution(piece):
        return pltpu.make_async_copy(cut(me, piece), laid(out_solution, me, piece), sol_own.at[piece])

    def own_before(piece):
        return pltpu.make_async_copy(cut(me - 1, piece), laid(before, me, piece), before_own.at[piece])

    def ship(piece):
        for k in others:
            group = pair ^ k
            late(piece, group, me, 2 * group + 1).start()

            def begin(parity, group=group):
                early(parity, piece, group, me, 2 * group, 2 * group + parity).start()

            on_parity(begin)

        def near(parity):
            to_partner(parity, piece, me).start()
            if parity:
                own_before(piece).start()
            else:
                late(piece, pair, me, partner).start()

        on_parity(near)
        own_solution(piece).start()

    def fd_copy(group, owner):
        return remote(
            fd.at[pl.ds(PAD, planes), pl.ds(PAD, block), 2 * group, :],
            out_defect.at[:, pl.ds(pl.multiple_of(snake(owner) * block, 8), block), :],
            fd_send.at[group], fd_recv.at[owner], 2 * group,
        )

    own_fd = pltpu.make_async_copy(
        fd.at[pl.ds(PAD, planes), pl.ds(PAD, block), me, :], out_defect.at[:, rows_of(me), :], fd_own
    )

    def outer_copy(side, dz):
        return pltpu.make_async_remote_copy(
            src_ref=out_solution.at[planes - 1 if dz > 0 else 0],
            dst_ref=outer.at[0 if dz > 0 else 1],
            send_sem=outer_send.at[side],
            recv_sem=outer_recv.at[side],
            device_id={"space": slab + dz},
            device_id_type=MESH,
        )

    own.wait()
    for k in order:
        inward(me, me ^ k, me ^ k).wait_recv()

    send(rhs, rhs, 2, 1, 0, peers)
    first = starter(a1, rhs, gain0)
    second = sweeper(a2, a1, None, gain0, hold0, peers)
    third = defecter(rhs1, a2, rhs, 1.0, peers, True)
    over(a1, 0, None, first)
    over(a2, -1, None, second)
    over(rhs1, -2, None, third)
    receive(0)
    over(a1, 2, 0, first)
    over(a2, 1, -1, second)
    over(rhs1, 0, -2, third)

    send(rhs1, rhs1, 2, 1, 1, half)
    send(a2, a3, 3, 2, 2, peers)
    first = starter(m1, rhs1, gain1, of_half)
    second = sweeper(m2, m1, None, gain1, hold1, half)
    third = defecter(scrap, m2, rhs1, 2.0, half, False)
    over(m1, 0, None, first)
    over(m2, -1, None, second)
    over(scrap, -2, None, third)
    receive(1)
    over(m1, 2, 0, first)
    over(m2, 1, -1, second)
    over(scrap, 0, -2, third)

    pairs = 2 * of_quarter

    def restrict(z, _):
        for x in range(half_block):
            zz, xx = 2 * z + PAD, 2 * x + PAD
            quad = (scrap[zz, xx] + scrap[zz + 1, xx]) + (
                scrap[zz, xx + 1] + scrap[zz + 1, xx + 1]
            )
            rhs2[z + PAD2, x + PAD2] = 0.25 * (pick(quad, pairs) + pick(quad, pairs + 1))
        return 0

    lax.fori_loop(0, half_planes, restrict, 0)
    send(rhs2, rhs2, 4, 4, 3, half // 2)
    send(m2, m3, 2, 1, 4, half)
    start = starter(k1, rhs2, gain2, of_quarter)
    second, third, fourth = (
        sweeper(new, old, first, gain2, hold2, half // 2, 4.0)
        for new, old, first in ((k2, k1, None), (k3, k2, k1), (k4, k3, k1))
    )
    over(k1, 0, None, start)
    over(k2, -1, None, second)
    receive(3)
    over(k1, 4, 0, start)
    over(k2, 3, -1, second)
    over(k3, 2, None, third)
    over(k4, 1, None, fourth)

    halved = of_half // 2

    def prolonger(received):
        def work(z, xs):
            for x in xs:
                value = pick(k4[z, x], halved)
                for dz in range(2):
                    for dx in range(2):
                        at = (2 * (z - PAD2) + dz + PAD, 2 * (x - PAD2) + dx + PAD)
                        base = pick(m3[at], of_half) if received else m2[at]
                        m3[at] = base + value

        return work

    over(k4, 0, None, prolonger(False))
    receive(4)
    over(k4, 1, 0, prolonger(True))
    over(m4, 1, None, sweeper(m4, m3, m1, gain1, hold1, half))
    over(m5, 0, None, sweeper(m5, m4, m1, gain1, hold1, half))
    send(m5, m5, 3, 2, 5, half)

    def joiner(base):
        def work(z, xs):
            for x in xs:
                a3[z, x] = base[z, x] + pick(m5[z, x], time // 2)

        return work

    fourth = sweeper(a4, a3, a1, gain0, hold0, peers)
    fifth = sweeper(a5, a4, a1, gain0, hold0, peers)
    last = defecter(fd, a5, rhs, 1.0, peers, False)
    over(a3, 0, None, joiner(a2))
    over(a4, -1, None, fourth)
    over(a5, -2, None, fifth)
    ship(0)
    over(fd, -3, None, last)
    receive(2)
    receive(5)
    over(a3, 3, 0, joiner(a3))
    over(a4, 2, -1, fourth)
    over(a5, 1, -2, fifth)
    for piece in range(1, 5):
        ship(piece)
    over(fd, 0, -3, last)
    for k in others:
        fd_copy(pair ^ k, me).start()
    pl.when(odd == 0)(own_fd.start)
    pl.when(odd == 1)(fd_copy(pair, me).start)

    def forward(parity):
        arrived_in = early
        for piece in range(5):
            for k in reversed(others):
                owner = 2 * (pair ^ k) + parity
                arrived_in(parity, piece, 0, owner, 2 * pair, me).wait_recv()
                relay(parity, piece, pair ^ k, owner).start()

    on_parity(forward)

    @pl.when(odd == 1)
    def _():
        for piece in (1, 2, 0, 3, 4):
            own_solution(piece).wait()
            for k in range(1, peers):
                late(piece, 0, me ^ k, me).wait_recv()
            if piece in (1, 2):
                side, dz = ((1, -1), (0, 1))[piece - 1]
                pl.when(has_z[dz])(outer_copy(side, dz).start)
        load_whole.wait()
        for piece in range(5):
            own_before(piece).wait()
            to_partner(0, piece, partner).wait_recv()
            for k in others:
                relay(0, piece, 0, 2 * (pair ^ k)).wait_recv()
        for side, dz in ((0, 1), (1, -1)):
            pl.when(has_z[-dz])(outer_copy(side, dz).wait_recv)
        row = lax.broadcasted_iota(jnp.int32, (rows, lanes), 0)
        column = lax.broadcasted_iota(jnp.int32, (rows, lanes), 1)
        for z in range(planes):
            centre = out_solution[z]
            across = (out_solution[z - 1] if z else outer[0]) + (
                out_solution[z + 1] if z < planes - 1 else outer[1]
            )
            across = across + (
                jnp.where(row > 0, pltpu.roll(centre, 1, 0), 0.0)
                + jnp.where(row < rows - 1, pltpu.roll(centre, rows - 1, 0), 0.0)
            )
            along = jnp.where(column > 0, pltpu.roll(centre, 1, 1), 0.0) + jnp.where(
                column < lanes - 1, pltpu.roll(centre, lanes - 1, 1), 0.0
            )
            left = (source[z] + before[z]) - centre
            out_defect[z] = left - conduct[z] * (2.0 * sum(FINE) * centre - (across + along))
        for side, dz in ((0, 1), (1, -1)):
            pl.when(has_z[dz])(outer_copy(side, dz).wait_send)

    @pl.when(odd == 0)
    def _():
        load_whole.wait()
        own_fd.wait()
        for piece in range(5):
            own_solution(piece).wait()
            late(piece, pair, me, partner).wait_send()
            to_partner(1, piece, partner).wait_recv()
            for k in others:
                relay(1, piece, 0, 2 * (pair ^ k) + 1).wait_recv()
        for k in range(1, peers):
            fd_copy(pair, me ^ k).wait_recv()

    for copies in started.values():
        for sends, _, copy in copies:
            pl.when(sends)(copy.wait_send)
    for side, dz in ((0, 1), (1, -1)):
        pl.when(has_z[dz])(cond_copy(side, dz).wait_send)
    for k in order:
        inward(me ^ k, me, me).wait_send()
    for k in others:
        fd_copy(pair ^ k, me).wait_send()
    pl.when(odd == 1)(fd_copy(pair, me).wait_send)

    def finish(parity):
        for piece in range(5):
            to_partner(parity, piece, me).wait_send()
            for k in others:
                late(piece, pair ^ k, me, me).wait_send()
                early(parity, piece, pair ^ k, me, 0, me).wait_send()
                relay(parity, piece, pair ^ k, 2 * (pair ^ k) + parity).wait_send()

    on_parity(finish)


def fused_body(peers, slabs, source, conductivity):
    _, planes, rows, lanes = source.shape
    block = rows // peers

    def field(depth, width):
        return pltpu.VMEM((depth, width, peers, lanes), jnp.float32)

    def table(depth, width):
        return pltpu.VMEM((depth, width, lanes), jnp.float32)

    large = field(planes + 2 * PAD, block + 2 * PAD)
    small = field(planes // 2 + 2 * PAD2, block // 2 + 2 * PAD2)
    fine = table(planes + 2 * PAD, block + 2 * NEAR)
    coarse = table(planes // 2 + 2 * PAD2, block // 2 + 2 * PAD2)
    dma = pltpu.SemaphoreType.DMA
    anywhere = pl.BlockSpec(memory_space=pl.ANY)
    local = pl.BlockSpec(memory_space=pltpu.VMEM)
    shape = pltpu.VMEM((planes, rows, lanes), jnp.float32)
    solution, final_defect = pl.pallas_call(
        functools.partial(cycle_kernel, peers, slabs),
        out_shape=(shape, shape),
        in_specs=[anywhere, anywhere],
        out_specs=(local, local),
        scratch_shapes=[
            large, large, small, large,
            table(planes + 2 * NEAR, block + 2 * NEAR),
            fine, fine, fine, fine, coarse, coarse,
            large, large, large, large, large, large,
            large, large, large, large, large,
            small, small, small, small,
            pltpu.VMEM((planes, rows, lanes), jnp.float32),
            pltpu.VMEM((planes, rows, lanes), jnp.float32),
            pltpu.VMEM((2, rows, lanes), jnp.float32),
            pltpu.VMEM((planes, rows, lanes), jnp.float32),
            dma((peers,)), dma((peers,)), dma, dma, dma((3,)), dma,
            dma((2,)), dma((2,)),
            dma((6, 8)), dma((6, 8)),
            dma((5, peers // 2)), dma((5, peers // 2)), dma((5,)), dma((5, peers // 2)),
            dma((5, peers)), dma((5, peers)), dma((5,)), dma((5,)),
            dma((peers // 2,)), dma((peers,)), dma, dma((2,)), dma((2,)),
        ],
        compiler_params=pltpu.CompilerParams(
            collective_id=0, has_side_effects=True, vmem_limit_bytes=56 * 1024 * 1024
        ),
    )(source[0], conductivity)
    return (solution[None], final_defect[None])


def solution(mesh):
    peers, slabs = mesh.shape["tm"], mesh.shape["space"]

    def chosen(source, conductivity):
        steps, planes, rows, lanes = source.shape
        if fits(steps * peers, peers, slabs, planes, rows, lanes):
            return fused_body(peers, slabs, source, conductivity)
        return body(source, conductivity)

    return jax.shard_map(
        chosen,
        mesh=mesh,
        in_specs=(P("tm", "space", None, None), P("space", None, None)),
        out_specs=(P("tm", "space", None, None), P("tm", "space", None, None)),
        check_vma=False,
    )
```

```python
import functools

import jax
import jax.numpy as jnp
from jax import lax
from jax.experimental import pallas as pl
from jax.experimental.pallas import tpu as pltpu
from jax.sharding import PartitionSpec as P

NU = 2
NC = 4


OMEGA = 0.8
FINE = (1.0, 1.0, 1.0)
COARSE = (0.25, 0.25, 1.0)


def padded_2(shard, sides, width):
    for axis, dim in sides:
        peers, length = (lax.axis_size(axis), shard.shape[dim])
        up = [(i, (i + 1) % peers) for i in range(peers - 1)]
        down = [(j, i) for i, j in up]
        last = lax.slice_in_dim(shard, length - width, length, axis=dim)
        first = lax.slice_in_dim(shard, 0, width, axis=dim)
        before = lax.ppermute(last, axis, up)
        after = lax.ppermute(first, axis, down)
        shard = jnp.concatenate([before, shard, after], axis=dim)
    return shard


def shifted(shard, axis, by):
    peers = lax.axis_size(axis)
    pairs = [(i, i + by) for i in range(peers) if 0 <= i + by < peers]
    return lax.ppermute(shard, axis, pairs)


def swapped(value, axis, bit):
    mask = 2**bit
    pairs = [(source, source ^ mask) for source in range(lax.axis_size(axis))]
    return lax.ppermute(value, axis, pairs)


def stencil(padded, weights):
    weight_z, weight_x, weight_y = weights
    centre = padded[1:-1, :, 1:-1]
    widened = jnp.pad(padded[1:-1], ((0, 0), (1, 1), (0, 0)))
    along_z = 2.0 * centre - padded[2:, :, 1:-1] - padded[:-2, :, 1:-1]
    along_x = 2.0 * centre - widened[:, 2:, 1:-1] - widened[:, :-2, 1:-1]
    along_y = 2.0 * centre - padded[1:-1, :, 2:] - padded[1:-1, :, :-2]
    return weight_z * along_z + weight_x * along_x + weight_y * along_y


def defect(current, right_side, earlier, padded, conduct, stretch, weights):
    applied = current + stretch * conduct * stencil(padded, weights)
    return right_side + earlier - applied


def relaxed(current, right_side, earlier, padded, conduct, stretch, weights):
    weight_sum = 2.0 * (weights[0] + weights[1] + weights[2])
    diagonal = 1.0 + stretch * conduct * weight_sum
    return (
        current
        + OMEGA * defect(current, right_side, earlier, padded, conduct, stretch, weights) / diagonal
    )


def coarsen(values):
    return 0.25 * (
        values[..., 0::2, 0::2, :]
        + values[..., 1::2, 0::2, :]
        + (values[..., 0::2, 1::2, :] + values[..., 1::2, 1::2, :])
    )


def refine(values):
    return jnp.repeat(jnp.repeat(values, 2, axis=-3), 2, axis=-2)


def zero_columns(values):
    return jnp.pad(values, ((0, 0), (0, 0), (1, 1)))


def plane_faces(values):
    return padded_2(values, (("space", 0),), 1)


def coarse_planes_framed(values):
    return padded_2(values, (("space", 0),), 1)


def fine_frame(values):
    return zero_columns(plane_faces(values))


def step_prior(values):
    return shifted(values, "tm", 1)


def pair_prior(values):
    return shifted(values, "tm", 2)


def group_prior(values):
    return shifted(values, "tm", 4)


def smooth(current, right_side, conduct, stretch, weights, repeats, earlier_of, framing):
    for turn_index in range(repeats):
        current = relaxed(
            current, right_side, earlier_of(current), framing(current), conduct, stretch, weights
        )
    return current


def body(source, conductivity):
    right_side = source[0]
    solution = smooth(
        jnp.zeros_like(right_side), right_side, conductivity, 1.0, FINE, NU, step_prior, fine_frame
    )
    defect_fine = defect(
        solution, right_side, step_prior(solution), fine_frame(solution), conductivity, 1.0, FINE
    )
    middle_full = defect_fine + swapped(defect_fine, "tm", 0)
    middle = smooth(
        jnp.zeros_like(middle_full),
        middle_full,
        conductivity,
        2.0,
        FINE,
        NU,
        pair_prior,
        fine_frame,
    )
    middle_defect = defect(
        middle, middle_full, pair_prior(middle), fine_frame(middle), conductivity, 2.0, FINE
    )
    summed = middle_defect + swapped(middle_defect, "tm", 1)
    coarse_rhs = coarsen(summed)
    coarse_cond = coarsen(conductivity)

    def coarse_frame(values):
        return zero_columns(coarse_planes_framed(values))

    coarse = smooth(
        jnp.zeros_like(coarse_rhs),
        coarse_rhs,
        coarse_cond,
        4.0,
        COARSE,
        NC,
        group_prior,
        coarse_frame,
    )
    middle = middle + refine(coarse)
    middle = smooth(middle, middle_full, conductivity, 2.0, FINE, NU, pair_prior, fine_frame)
    solution = solution + middle
    solution = smooth(solution, right_side, conductivity, 1.0, FINE, NU, step_prior, fine_frame)
    final_defect = defect(
        solution, right_side, step_prior(solution), fine_frame(solution), conductivity, 1.0, FINE
    )
    return (solution[None], final_defect[None])


MESH = pl.DeviceIdType.MESH


def snake(index):
    return index + ((index // 2) % 2) * (1 - 2 * (index % 2))


def scaled(weights, stretch):
    return tuple(stretch * weight for weight in weights)


def fits(steps, peers, slabs, planes, rows, lanes):
    block = rows // peers
    return (
        steps == peers
        and peers % 8 == 0
        and peers & (peers - 1) == 0
        and rows % peers == 0
        and block % 8 == 0
        and planes % 2 == 0
        and planes >= 8
        and lanes % 128 == 0
        and peers == 8
        and slabs > 1
    )


PAD, PAD2 = 4, 4
NEAR = 2 * PAD2
UNROLL = 160


def cycle_kernel(
    peers,
    slabs,
    source_far,
    conduct_far,
    out_solution,
    out_defect,
    rhs, rhs1, rhs2, scrap,
    cond, inner, gain0, hold0, gain1, hold1, gain2, hold2,
    a1, a2, a3, a4, a5, fd,
    m1, m2, m3, m4, m5,
    k1, k2, k3, k4,
    source, before, outer, conduct,
    in_send, in_recv, own_sem, load_sem, cond_load, conduct_load,
    cond_send, cond_recv,
    h_send, h_recv,
    late_send, early_send, pair_send, relay_send, sol_recv, before_recv,
    sol_own, before_own, fd_send, fd_recv, fd_own, outer_send, outer_recv,
):
    planes, rows, lanes = source.shape
    block = rows // peers
    half_planes, half_block = planes // 2, block // 2
    me, slab = lax.axis_index("tm"), lax.axis_index("space")
    mine = snake(me)
    following, preceding = snake((mine + 1) % peers), snake((mine + peers - 1) % peers)
    has_z = {1: slab < slabs - 1, -1: slab > 0, 0: None}
    has_x = {1: mine < peers - 1, -1: mine > 0, 0: None}
    beside = {1: following, -1: preceding}

    def both(first, second):
        if first is None:
            return second
        return first if second is None else first & second

    def device(dz, dx):
        where = {}
        if dx:
            where["tm"] = beside[dx]
        if dz:
            where["space"] = slab + dz
        return where

    def size_of(ref):
        pad = PAD2 if ref.shape[0] == half_planes + 2 * PAD2 else PAD
        return pad, ref.shape[0] - 2 * pad, ref.shape[1] - 2 * pad

    def over(ref, outer, inner, work):
        pad, depth, width = size_of(ref)
        z0, z1, x0, x1 = pad - outer, pad + depth + outer, pad - outer, pad + width + outer
        parts = []
        if inner is None:
            parts.append((z0, z1, list(range(x0, x1))))
        else:
            i0, i1, j0, j1 = pad - inner, pad + depth + inner, pad - inner, pad + width + inner
            parts.append((z0, i0, list(range(x0, x1))))
            parts.append((i1, z1, list(range(x0, x1))))
            parts.append((i0, i1, list(range(x0, j0)) + list(range(j1, x1))))
        over_parts(parts, work)

    def over_parts(parts, work):
        for first, last, xs in parts:
            count = last - first
            if count <= 0 or not xs:
                continue
            folds = [u for u in range(1, count + 1) if count % u == 0 and u * len(xs) <= UNROLL]
            fold = max(folds) if folds else 1
            if fold == count:
                for z in range(first, last):
                    work(z, xs)
                continue

            def step(i, _, first=first, xs=xs, fold=fold):
                for u in range(fold):
                    work(first + i * fold + u, xs)
                return 0

            lax.fori_loop(0, count // fold, step, 0)

    load_source = pltpu.make_async_copy(source_far, source, load_sem)
    load_source.start()

    def window(number):
        start, count, at = ((0, block, NEAR), (-NEAR, NEAR, 0), (block, NEAR, NEAR + block))[number]
        return pltpu.make_async_copy(
            conduct_far.at[:, pl.ds(pl.multiple_of(mine * block + start, 8), count), :],
            cond.at[pl.ds(NEAR, planes), pl.ds(at, count), :],
            cond_load.at[number],
        )

    load_whole = pltpu.make_async_copy(conduct_far, conduct, conduct_load)
    window(0).start()
    pl.when(has_x[-1])(window(1).start)
    pl.when(has_x[1])(window(2).start)

    barrier = pltpu.get_barrier_semaphore()
    for k in range(1, peers):
        pl.semaphore_signal(barrier, inc=1, device_id={"tm": me ^ k}, device_id_type=MESH)
    expected = peers - 1
    for dz in (1, -1):
        for dx in (0, 1, -1):
            here = both(has_z[dz], has_x[dx])

            @pl.when(here)
            def _(dz=dz, dx=dx):
                pl.semaphore_signal(
                    barrier, inc=1, device_id=device(dz, dx), device_id_type=MESH
                )

            expected = expected + jnp.where(here, 1, 0)
    load_source.wait()
    pl.semaphore_wait(barrier, expected)

    def rows_of(index):
        return pl.ds(pl.multiple_of(snake(index) * block, 8), block)

    def inward(peer, step, recv):
        return pltpu.make_async_remote_copy(
            src_ref=source.at[:, rows_of(peer), :],
            dst_ref=rhs.at[pl.ds(PAD, planes), pl.ds(PAD, block), step, :],
            send_sem=in_send.at[peer],
            recv_sem=in_recv.at[recv],
            device_id={"tm": peer},
            device_id_type=MESH,
        )

    order = sorted(range(1, peers), reverse=True)
    for k in order:
        inward(me ^ k, me, me).start()
    own = pltpu.make_async_copy(
        source_far.at[:, rows_of(me), :],
        rhs.at[pl.ds(PAD, planes), pl.ds(PAD, block), me, :],
        own_sem,
    )
    own.start()
    load_whole.start()
    window(0).wait()
    pl.when(has_x[-1])(window(1).wait)
    pl.when(has_x[1])(window(2).wait)

    def cond_copy(side, dz):
        return pltpu.make_async_remote_copy(
            src_ref=cond.at[pl.ds(planes, NEAR) if dz > 0 else pl.ds(NEAR, NEAR)],
            dst_ref=cond.at[pl.ds(0, NEAR) if dz > 0 else pl.ds(NEAR + planes, NEAR)],
            send_sem=cond_send.at[side],
            recv_sem=cond_recv.at[side],
            device_id={"space": slab + dz},
            device_id_type=MESH,
        )

    for side, dz in ((0, 1), (1, -1)):
        pl.when(has_z[dz])(cond_copy(side, dz).start)

    for side, dz in ((0, -1), (1, 1)):

        @pl.when(jnp.logical_not(has_z[dz]))
        def _(side=side):
            outer[side] = jnp.zeros((rows, lanes), jnp.float32)

    for ref in (rhs, m3, m5, rhs2):
        pad, deep, broad = size_of(ref)
        for dz, first in ((-1, 0), (1, pad + deep)):

            @pl.when(jnp.logical_not(has_z[dz]))
            def _(ref=ref, first=first, pad=pad):
                def clear(z, _):
                    ref[z] = jnp.zeros(ref.shape[1:], jnp.float32)
                    return 0

                lax.fori_loop(first, first + pad, clear, 0)

        for dx, first in ((-1, 0), (1, pad + broad)):

            @pl.when(jnp.logical_not(has_x[dx]))
            def _(ref=ref, first=first, pad=pad):
                def clear(z, _):
                    ref[z, first : first + pad] = jnp.zeros((pad, peers, lanes), jnp.float32)
                    return 0

                lax.fori_loop(0, ref.shape[0], clear, 0)

    for side, dz in ((0, 1), (1, -1)):
        pl.when(has_z[-dz])(cond_copy(side, dz).wait_recv)

    def fill(z, _):
        plane = slab * planes + z - PAD
        deep = (plane >= 0) & (plane < slabs * planes)
        for part in range((block + 2 * NEAR) // 8):
            at = pl.ds(8 * part, 8)
            row = mine * block - NEAR + 8 * part + lax.broadcasted_iota(jnp.int32, (8, lanes), 0)
            ok = deep & (row >= 0) & (row < rows)
            value = jnp.where(ok, cond[z - PAD + NEAR, at, :], 0.0)
            fine = jnp.where(ok, OMEGA / (1.0 + value * (2.0 * sum(FINE))), 0.0)
            middle = jnp.where(ok, OMEGA / (1.0 + value * (4.0 * sum(FINE))), 0.0)
            inner[z, at, :] = value
            gain0[z, at, :] = fine
            hold0[z, at, :] = fine * value
            gain1[z, at, :] = middle
            hold1[z, at, :] = middle * (2.0 * value)
        return 0

    lax.fori_loop(0, planes + 2 * PAD, fill, 0)

    def fill2(z, _):
        plane = slab * half_planes + z - PAD2
        deep = (plane >= 0) & (plane < slabs * half_planes)
        for part in range((block + 2 * NEAR) // 16):
            at = pl.ds(8 * part, 8)
            even, odd = pl.ds(16 * part, 8, stride=2), pl.ds(16 * part + 1, 8, stride=2)
            quad = (cond[2 * z, even, :] + cond[2 * z + 1, even, :]) + (
                cond[2 * z, odd, :] + cond[2 * z + 1, odd, :]
            )
            row = mine * half_block - PAD2 + 8 * part
            row = row + lax.broadcasted_iota(jnp.int32, (8, lanes), 0)
            ok = deep & (row >= 0) & (row < rows // 2)
            value = jnp.where(ok, 0.25 * quad, 0.0)
            gain = jnp.where(ok, OMEGA / (1.0 + value * (8.0 * sum(COARSE))), 0.0)
            gain2[z, at, :] = gain
            hold2[z, at, :] = gain * value
        return 0

    lax.fori_loop(0, half_planes + 2 * PAD2, fill2, 0)

    time = lax.broadcasted_iota(jnp.int32, (peers, lanes), 0)
    lane = lax.broadcasted_iota(jnp.int32, (peers, lanes), 1)
    not_first, not_last = lane > 0, lane < lanes - 1
    later = {count: time % count > 0 for count in (peers, peers // 2, peers // 4)}

    def pick(value, index):
        return jnp.take_along_axis(value, index, axis=0, mode="promise_in_bounds")

    def prior(value, steps):
        return jnp.where(later[steps], pltpu.roll(value, 1, 0), 0.0)

    def spread(ref, z, x, pad):
        near = PAD2 if ref.shape[1] == half_block + 2 * PAD2 else NEAR
        return jnp.broadcast_to(ref[z, pl.ds(x - pad + near, 1), :], (peers, lanes))

    def around(ref, z, xs, weight_y):
        wanted = sorted({x + step for x in xs for step in (-1, 0, 1)})
        row = {x: ref[z, x] for x in wanted}
        for x in xs:
            centre = row[x]
            across = (ref[z - 1, x] + ref[z + 1, x]) + (row[x - 1] + row[x + 1])
            along = jnp.where(not_first, pltpu.roll(centre, 1, 1), 0.0) + jnp.where(
                not_last, pltpu.roll(centre, lanes - 1, 1), 0.0
            )
            total = across + along if weight_y == 1.0 else across + weight_y * along
            yield x, centre, total

    def sweeper(new, old, first, gain, hold, steps, weight_y=1.0):
        pad = size_of(new)[0]

        def work(z, xs):
            for x, centre, total in around(old, z, xs, weight_y):
                if first is None:
                    value = (2.0 - OMEGA) * centre
                else:
                    value = (1.0 - OMEGA) * centre + first[z, x]
                value = value + spread(gain, z, x, pad) * prior(centre, steps)
                new[z, x] = value + spread(hold, z, x, pad) * total

        return work

    def starter(new, right, gain, index=None):
        pad = size_of(new)[0]

        def work(z, xs):
            for x in xs:
                value = right[z, x] if index is None else pick(right[z, x], index)
                new[z, x] = spread(gain, z, x, pad) * value

        return work

    def defecter(new, old, right, stretch, steps, paired):
        def work(z, xs):
            for x, centre, total in around(old, z, xs, 1.0):
                value = spread(inner, z, x, PAD)
                if stretch != 1.0:
                    value = stretch * value
                left = (right[z, x] + prior(centre, steps)) - centre
                left = left - value * (2.0 * sum(FINE) * centre - total)
                if paired:
                    left = pick(left, evens) + pick(left, evens + 1)
                new[z, x] = left

        return work

    half = peers // 2
    of_half, of_quarter = time % half, time % (half // 2)
    evens = 2 * of_half

    def wide(ref, into, layers, corner_layers, stage, steps):
        pad, deep, broad = size_of(ref)

        def spans(step, size, span):
            low, high = span
            if step == 0:
                return pl.ds(pad, size), pl.ds(pad, size)
            if step > 0:
                return pl.ds(pad + size - high, high - low), pl.ds(pad - high, high - low)
            return pl.ds(pad + low, high - low), pl.ds(pad + size + low, high - low)

        blocks = [
            (dz, dx, *ranges) for ranges in corner_layers for dz in (1, -1) for dx in (1, -1)
        ]
        blocks += [(dz, dx, layers, layers) for dz, dx in ((0, 1), (0, -1), (1, 0), (-1, 0))]
        out = []
        for number, (dz, dx, z_span, x_span) in enumerate(blocks):
            src_z, dst_z = spans(dz, deep, z_span)
            src_x, dst_x = spans(dx, broad, x_span)
            some = () if steps == peers else (pl.ds(0, steps),)
            copy = pltpu.make_async_remote_copy(
                src_ref=ref.at[(src_z, src_x, *some)],
                dst_ref=into.at[(dst_z, dst_x, *some)],
                send_sem=h_send.at[stage, number],
                recv_sem=h_recv.at[stage, number],
                device_id=device(dz, dx),
                device_id_type=MESH,
            )
            sends = both(has_z[dz], has_x[dx])
            arrives = both(has_z[-dz], has_x[-dx])
            out.append((sends, arrives, copy))
        return out

    started = {}

    def send(ref, into, layers, corner_layers, stage, steps):
        started[stage] = wide(ref, into, layers, corner_layers, stage, steps)
        for sends, _, copy in started[stage]:
            pl.when(sends)(copy.start)

    def square(depth):
        return (((0, depth), (0, depth)),)

    def receive(stage):
        for _, arrives, copy in started[stage]:
            pl.when(arrives)(copy.wait_recv)

    def pieces_of(ref, edge):
        _, deep, broad = size_of(ref)
        return (
            (edge, deep - 2 * edge, edge, broad - 2 * edge),
            (0, edge, 0, broad),
            (deep - edge, edge, 0, broad),
            (edge, deep - 2 * edge, 0, edge),
            (edge, deep - 2 * edge, broad - edge, edge),
        )

    parts = pieces_of(a5, 2)
    pair, odd = me // 2, me % 2
    partner = me + 1 - 2 * odd
    others = sorted(range(1, peers // 2), reverse=True)

    def on_parity(work):
        pl.when(odd == 0)(functools.partial(work, 0))
        pl.when(odd == 1)(functools.partial(work, 1))

    def cut(step, piece):
        z, deep, x, broad = parts[piece]
        return a5.at[pl.ds(z + PAD, deep), pl.ds(x + PAD, broad), step, :]

    def laid(ref, owner, piece):
        z, deep, x, broad = parts[piece]
        return ref.at[pl.ds(z, deep), pl.ds(snake(owner) * block + x, broad), :]

    def place(parity):
        return (before, before_recv) if parity else (out_solution, sol_recv)

    def remote(src, dst, send_sem, recv_sem, peer):
        return pltpu.make_async_remote_copy(
            src_ref=src,
            dst_ref=dst,
            send_sem=send_sem,
            recv_sem=recv_sem,
            device_id={"tm": peer},
            device_id_type=MESH,
        )

    def late(piece, group, owner, peer):
        return remote(
            cut(peer, piece), laid(out_solution, owner, piece),
            late_send.at[piece, group], sol_recv.at[piece, owner], peer,
        )

    def early(parity, piece, group, owner, step, peer):
        into, arrived = place(parity)
        return remote(
            cut(step, piece), laid(into, owner, piece),
            early_send.at[piece, group], arrived.at[piece, owner], peer,
        )

    def to_partner(parity, piece, owner):
        into, arrived = place(1 - parity)
        return remote(
            cut(2 * pair, piece), laid(into, owner, piece),
            pair_send.at[piece], arrived.at[piece, owner], partner,
        )

    def relay(parity, piece, group, owner):
        source_of = place(parity)[0]
        into, arrived = place(1 - parity)
        return remote(
            laid(source_of, owner, piece), laid(into, owner, piece),
            relay_send.at[piece, group], arrived.at[piece, owner], partner,
        )

    def own_solution(piece):
        return pltpu.make_async_copy(cut(me, piece), laid(out_solution, me, piece), sol_own.at[piece])

    def own_before(piece):
        return pltpu.make_async_copy(cut(me - 1, piece), laid(before, me, piece), before_own.at[piece])

    def ship(piece):
        for k in others:
            group = pair ^ k
            late(piece, group, me, 2 * group + 1).start()

            def begin(parity, group=group):
                early(parity, piece, group, me, 2 * group, 2 * group + parity).start()

            on_parity(begin)

        def near(parity):
            to_partner(parity, piece, me).start()
            if parity:
                own_before(piece).start()
            else:
                late(piece, pair, me, partner).start()

        on_parity(near)
        own_solution(piece).start()

    def fd_copy(group, owner):
        return remote(
            fd.at[pl.ds(PAD, planes), pl.ds(PAD, block), 2 * group, :],
            out_defect.at[:, pl.ds(pl.multiple_of(snake(owner) * block, 8), block), :],
            fd_send.at[group], fd_recv.at[owner], 2 * group,
        )

    own_fd = pltpu.make_async_copy(
        fd.at[pl.ds(PAD, planes), pl.ds(PAD, block), me, :], out_defect.at[:, rows_of(me), :], fd_own
    )

    def outer_copy(side, dz):
        return pltpu.make_async_remote_copy(
            src_ref=out_solution.at[planes - 1 if dz > 0 else 0],
            dst_ref=outer.at[0 if dz > 0 else 1],
            send_sem=outer_send.at[side],
            recv_sem=outer_recv.at[side],
            device_id={"space": slab + dz},
            device_id_type=MESH,
        )

    own.wait()
    for k in order:
        inward(me, me ^ k, me ^ k).wait_recv()

    send(rhs, rhs, (0, 2), square(1), 0, peers)
    send(rhs, rhs, (2, 4), (((0, 1), (1, 3)), ((1, 3), (0, 2))), 1, peers)
    first = starter(a1, rhs, gain0)
    second = sweeper(a2, a1, None, gain0, hold0, peers)
    third = defecter(rhs1, a2, rhs, 1.0, peers, True)
    over(a1, 0, None, first)
    over(a2, -1, None, second)
    over(rhs1, -2, None, third)
    receive(0)
    top, left = PAD + planes, PAD + block
    inside = list(range(PAD, left))
    flank = [PAD - 2, PAD - 1, left, left + 1]
    over_parts(
        [(PAD - 2, PAD, inside), (top, top + 2, inside), (PAD, top, flank)]
        + [(z, z + 1, [PAD - 1, left]) for z in (PAD - 1, top)],
        first,
    )
    middle_rows = [PAD - 1, *inside, left]
    over_parts(
        [(PAD - 1, PAD, inside), (PAD, PAD + 1, middle_rows)]
        + [(top - 1, top, middle_rows), (top, top + 1, inside)]
        + [(PAD + 1, top - 1, [PAD - 1, PAD, left - 1, left])],
        second,
    )
    over(rhs1, 0, -2, third)
    fourth = starter(m1, rhs1, gain1)
    fifth = sweeper(m2, m1, None, gain1, hold1, half)
    sixth = defecter(scrap, m2, rhs1, 2.0, half, False)
    over(m1, 0, None, fourth)
    over(m2, -1, None, fifth)
    over(scrap, -2, None, sixth)
    receive(1)
    for z in (PAD - 2, PAD - 1, top, top + 1):
        first(z, flank)
    over(a1, 4, 2, first)
    for z in (PAD - 1, top):
        second(z, [PAD - 1, left])
    over(a2, 3, 1, second)
    over(rhs1, 2, 0, third)
    over(m1, 2, 0, fourth)
    over(m2, 1, -1, fifth)
    over(scrap, 0, -2, sixth)

    pairs = 2 * of_quarter

    def restrict(z, _):
        for x in range(half_block):
            zz, xx = 2 * z + PAD, 2 * x + PAD
            quad = (scrap[zz, xx] + scrap[zz + 1, xx]) + (
                scrap[zz, xx + 1] + scrap[zz + 1, xx + 1]
            )
            rhs2[z + PAD2, x + PAD2] = 0.25 * (pick(quad, pairs) + pick(quad, pairs + 1))
        return 0

    lax.fori_loop(0, half_planes, restrict, 0)
    send(rhs2, rhs2, (0, 4), square(4), 3, half // 2)
    send(m2, m3, (0, 2), square(1), 4, half)
    start = starter(k1, rhs2, gain2, of_quarter)
    second, third, fourth = (
        sweeper(new, old, first, gain2, hold2, half // 2, 4.0)
        for new, old, first in ((k2, k1, None), (k3, k2, k1), (k4, k3, k1))
    )
    over(k1, 0, None, start)
    over(k2, -1, None, second)
    receive(3)
    over(k1, 4, 0, start)
    over(k2, 3, -1, second)
    over(k3, 2, None, third)
    over(k4, 1, None, fourth)

    halved = of_half // 2

    def prolonger(received):
        def work(z, xs):
            for x in xs:
                value = pick(k4[z, x], halved)
                for dz in range(2):
                    for dx in range(2):
                        at = (2 * (z - PAD2) + dz + PAD, 2 * (x - PAD2) + dx + PAD)
                        base = pick(m3[at], of_half) if received else m2[at]
                        m3[at] = base + value

        return work

    over(k4, 0, None, prolonger(False))
    receive(4)
    over(k4, 1, 0, prolonger(True))
    over(m4, 1, None, sweeper(m4, m3, m1, gain1, hold1, half))
    over(m5, 0, None, sweeper(m5, m4, m1, gain1, hold1, half))
    send(m5, m5, (0, 3), square(2), 5, half)

    def joiner(base):
        def work(z, xs):
            for x in xs:
                a3[z, x] = base[z, x] + pick(m5[z, x], time // 2)

        return work

    fourth = sweeper(a4, a3, a1, gain0, hold0, peers)
    fifth = sweeper(a5, a4, a1, gain0, hold0, peers)
    last = defecter(fd, a5, rhs, 1.0, peers, False)
    over(a3, 0, None, joiner(a2))
    over(a4, -1, None, fourth)
    over(a5, -2, None, fifth)
    ship(0)
    over(fd, -3, None, last)
    receive(5)
    over(a3, 3, 0, joiner(a2))
    over(a4, 2, -1, fourth)
    over(a5, 1, -2, fifth)
    for piece in range(1, 5):
        ship(piece)
    over(fd, 0, -3, last)
    for k in others:
        fd_copy(pair ^ k, me).start()
    pl.when(odd == 0)(own_fd.start)
    pl.when(odd == 1)(fd_copy(pair, me).start)

    def forward(parity):
        for piece in (0, 1, 2, None, 3, 4):
            if piece is None:
                if parity:
                    for edge, side, dz in ((1, 1, -1), (2, 0, 1)):
                        own_solution(edge).wait()
                        for k in range(1, peers):
                            late(edge, 0, me ^ k, me).wait_recv()
                        pl.when(has_z[dz])(outer_copy(side, dz).start)
                continue
            for k in reversed(others):
                owner = 2 * (pair ^ k) + parity
                early(parity, piece, 0, owner, 2 * pair, me).wait_recv()
                relay(parity, piece, pair ^ k, owner).start()

    on_parity(forward)

    @pl.when(odd == 1)
    def _():
        for piece in (0, 3, 4):
            own_solution(piece).wait()
            for k in range(1, peers):
                late(piece, 0, me ^ k, me).wait_recv()
        load_whole.wait()
        row = lax.broadcasted_iota(jnp.int32, (rows, lanes), 0)
        column = lax.broadcasted_iota(jnp.int32, (rows, lanes), 1)
        for z in (*range(1, planes - 1), None, 0, planes - 1):
            if z is None:
                for side, dz in ((0, 1), (1, -1)):
                    pl.when(has_z[-dz])(outer_copy(side, dz).wait_recv)
                continue
            centre = out_solution[z]
            across = (out_solution[z - 1] if z else outer[0]) + (
                out_solution[z + 1] if z < planes - 1 else outer[1]
            )
            across = across + (
                jnp.where(row > 0, pltpu.roll(centre, 1, 0), 0.0)
                + jnp.where(row < rows - 1, pltpu.roll(centre, rows - 1, 0), 0.0)
            )
            along = jnp.where(column > 0, pltpu.roll(centre, 1, 1), 0.0) + jnp.where(
                column < lanes - 1, pltpu.roll(centre, lanes - 1, 1), 0.0
            )
            left = source[z] - centre
            out_defect[z] = left - conduct[z] * (2.0 * sum(FINE) * centre - (across + along))
        for piece in range(5):
            own_before(piece).wait()
            to_partner(0, piece, partner).wait_recv()
            for k in others:
                relay(0, piece, 0, 2 * (pair ^ k)).wait_recv()
        for z in range(planes):
            out_defect[z] = out_defect[z] + before[z]
        for side, dz in ((0, 1), (1, -1)):
            pl.when(has_z[dz])(outer_copy(side, dz).wait_send)

    @pl.when(odd == 0)
    def _():
        load_whole.wait()
        own_fd.wait()
        for piece in range(5):
            own_solution(piece).wait()
            late(piece, pair, me, partner).wait_send()
            to_partner(1, piece, partner).wait_recv()
            for k in others:
                relay(1, piece, 0, 2 * (pair ^ k) + 1).wait_recv()
        for k in range(1, peers):
            fd_copy(pair, me ^ k).wait_recv()

    for copies in started.values():
        for sends, _, copy in copies:
            pl.when(sends)(copy.wait_send)
    for side, dz in ((0, 1), (1, -1)):
        pl.when(has_z[dz])(cond_copy(side, dz).wait_send)
    for k in order:
        inward(me ^ k, me, me).wait_send()
    for k in others:
        fd_copy(pair ^ k, me).wait_send()
    pl.when(odd == 1)(fd_copy(pair, me).wait_send)

    def finish(parity):
        for piece in range(5):
            to_partner(parity, piece, me).wait_send()
            for k in others:
                late(piece, pair ^ k, me, me).wait_send()
                early(parity, piece, pair ^ k, me, 0, me).wait_send()
                relay(parity, piece, pair ^ k, 2 * (pair ^ k) + parity).wait_send()

    on_parity(finish)


def fused_body(peers, slabs, source, conductivity):
    _, planes, rows, lanes = source.shape
    block = rows // peers

    def field(depth, width):
        return pltpu.VMEM((depth, width, peers, lanes), jnp.float32)

    def table(depth, width):
        return pltpu.VMEM((depth, width, lanes), jnp.float32)

    large = field(planes + 2 * PAD, block + 2 * PAD)
    small = field(planes // 2 + 2 * PAD2, block // 2 + 2 * PAD2)
    fine = table(planes + 2 * PAD, block + 2 * NEAR)
    coarse = table(planes // 2 + 2 * PAD2, block // 2 + 2 * PAD2)
    dma = pltpu.SemaphoreType.DMA
    anywhere = pl.BlockSpec(memory_space=pl.ANY)
    local = pl.BlockSpec(memory_space=pltpu.VMEM)
    shape = pltpu.VMEM((planes, rows, lanes), jnp.float32)
    solution, final_defect = pl.pallas_call(
        functools.partial(cycle_kernel, peers, slabs),
        out_shape=(shape, shape),
        in_specs=[anywhere, anywhere],
        out_specs=(local, local),
        scratch_shapes=[
            large, large, small, large,
            table(planes + 2 * NEAR, block + 2 * NEAR),
            fine, fine, fine, fine, fine, coarse, coarse,
            large, large, large, large, large, large,
            large, large, large, large, large,
            small, small, small, small,
            pltpu.VMEM((planes, rows, lanes), jnp.float32),
            pltpu.VMEM((planes, rows, lanes), jnp.float32),
            pltpu.VMEM((2, rows, lanes), jnp.float32),
            pltpu.VMEM((planes, rows, lanes), jnp.float32),
            dma((peers,)), dma((peers,)), dma, dma, dma((3,)), dma,
            dma((2,)), dma((2,)),
            dma((6, 12)), dma((6, 12)),
            dma((5, peers // 2)), dma((5, peers // 2)), dma((5,)), dma((5, peers // 2)),
            dma((5, peers)), dma((5, peers)), dma((5,)), dma((5,)),
            dma((peers // 2,)), dma((peers,)), dma, dma((2,)), dma((2,)),
        ],
        compiler_params=pltpu.CompilerParams(
            collective_id=0, has_side_effects=True, vmem_limit_bytes=56 * 1024 * 1024
        ),
    )(source[0], conductivity)
    return (solution[None], final_defect[None])


def solution(mesh):
    peers, slabs = mesh.shape["tm"], mesh.shape["space"]

    def chosen(source, conductivity):
        steps, planes, rows, lanes = source.shape
        if fits(steps * peers, peers, slabs, planes, rows, lanes):
            return fused_body(peers, slabs, source, conductivity)
        return body(source, conductivity)

    return jax.shard_map(
        chosen,
        mesh=mesh,
        in_specs=(P("tm", "space", None, None), P("space", None, None)),
        out_specs=(P("tm", "space", None, None), P("tm", "space", None, None)),
        check_vma=False,
    )
```

```python
import functools

import jax
import jax.numpy as jnp
from jax import lax
from jax.experimental import pallas as pl
from jax.experimental.pallas import tpu as pltpu
from jax.sharding import PartitionSpec as P

NU = 2
NC = 4


OMEGA = 0.8
FINE = (1.0, 1.0, 1.0)
COARSE = (0.25, 0.25, 1.0)


def padded_2(shard, sides, width):
    for axis, dim in sides:
        peers, length = (lax.axis_size(axis), shard.shape[dim])
        up = [(i, (i + 1) % peers) for i in range(peers - 1)]
        down = [(j, i) for i, j in up]
        last = lax.slice_in_dim(shard, length - width, length, axis=dim)
        first = lax.slice_in_dim(shard, 0, width, axis=dim)
        before = lax.ppermute(last, axis, up)
        after = lax.ppermute(first, axis, down)
        shard = jnp.concatenate([before, shard, after], axis=dim)
    return shard


def shifted(shard, axis, by):
    peers = lax.axis_size(axis)
    pairs = [(i, i + by) for i in range(peers) if 0 <= i + by < peers]
    return lax.ppermute(shard, axis, pairs)


def swapped(value, axis, bit):
    mask = 2**bit
    pairs = [(source, source ^ mask) for source in range(lax.axis_size(axis))]
    return lax.ppermute(value, axis, pairs)


def stencil(padded, weights):
    weight_z, weight_x, weight_y = weights
    centre = padded[1:-1, :, 1:-1]
    widened = jnp.pad(padded[1:-1], ((0, 0), (1, 1), (0, 0)))
    along_z = 2.0 * centre - padded[2:, :, 1:-1] - padded[:-2, :, 1:-1]
    along_x = 2.0 * centre - widened[:, 2:, 1:-1] - widened[:, :-2, 1:-1]
    along_y = 2.0 * centre - padded[1:-1, :, 2:] - padded[1:-1, :, :-2]
    return weight_z * along_z + weight_x * along_x + weight_y * along_y


def defect(current, right_side, earlier, padded, conduct, stretch, weights):
    applied = current + stretch * conduct * stencil(padded, weights)
    return right_side + earlier - applied


def relaxed(current, right_side, earlier, padded, conduct, stretch, weights):
    weight_sum = 2.0 * (weights[0] + weights[1] + weights[2])
    diagonal = 1.0 + stretch * conduct * weight_sum
    return (
        current
        + OMEGA * defect(current, right_side, earlier, padded, conduct, stretch, weights) / diagonal
    )


def coarsen(values):
    return 0.25 * (
        values[..., 0::2, 0::2, :]
        + values[..., 1::2, 0::2, :]
        + (values[..., 0::2, 1::2, :] + values[..., 1::2, 1::2, :])
    )


def refine(values):
    return jnp.repeat(jnp.repeat(values, 2, axis=-3), 2, axis=-2)


def zero_columns(values):
    return jnp.pad(values, ((0, 0), (0, 0), (1, 1)))


def plane_faces(values):
    return padded_2(values, (("space", 0),), 1)


def coarse_planes_framed(values):
    return padded_2(values, (("space", 0),), 1)


def fine_frame(values):
    return zero_columns(plane_faces(values))


def step_prior(values):
    return shifted(values, "tm", 1)


def pair_prior(values):
    return shifted(values, "tm", 2)


def group_prior(values):
    return shifted(values, "tm", 4)


def smooth(current, right_side, conduct, stretch, weights, repeats, earlier_of, framing):
    for turn_index in range(repeats):
        current = relaxed(
            current, right_side, earlier_of(current), framing(current), conduct, stretch, weights
        )
    return current


def body(source, conductivity):
    right_side = source[0]
    solution = smooth(
        jnp.zeros_like(right_side), right_side, conductivity, 1.0, FINE, NU, step_prior, fine_frame
    )
    defect_fine = defect(
        solution, right_side, step_prior(solution), fine_frame(solution), conductivity, 1.0, FINE
    )
    middle_full = defect_fine + swapped(defect_fine, "tm", 0)
    middle = smooth(
        jnp.zeros_like(middle_full),
        middle_full,
        conductivity,
        2.0,
        FINE,
        NU,
        pair_prior,
        fine_frame,
    )
    middle_defect = defect(
        middle, middle_full, pair_prior(middle), fine_frame(middle), conductivity, 2.0, FINE
    )
    summed = middle_defect + swapped(middle_defect, "tm", 1)
    coarse_rhs = coarsen(summed)
    coarse_cond = coarsen(conductivity)

    def coarse_frame(values):
        return zero_columns(coarse_planes_framed(values))

    coarse = smooth(
        jnp.zeros_like(coarse_rhs),
        coarse_rhs,
        coarse_cond,
        4.0,
        COARSE,
        NC,
        group_prior,
        coarse_frame,
    )
    middle = middle + refine(coarse)
    middle = smooth(middle, middle_full, conductivity, 2.0, FINE, NU, pair_prior, fine_frame)
    solution = solution + middle
    solution = smooth(solution, right_side, conductivity, 1.0, FINE, NU, step_prior, fine_frame)
    final_defect = defect(
        solution, right_side, step_prior(solution), fine_frame(solution), conductivity, 1.0, FINE
    )
    return (solution[None], final_defect[None])


MESH = pl.DeviceIdType.MESH


def snake(index):
    return index + ((index // 2) % 2) * (1 - 2 * (index % 2))


def scaled(weights, stretch):
    return tuple(stretch * weight for weight in weights)


def fits(steps, peers, slabs, planes, rows, lanes):
    block = rows // peers
    return (
        steps == peers
        and peers % 8 == 0
        and peers & (peers - 1) == 0
        and rows % peers == 0
        and block % 8 == 0
        and planes % 2 == 0
        and planes >= 8
        and lanes % 128 == 0
        and peers == 8
        and slabs > 1
    )


PAD, PAD2 = 4, 4
NEAR = 2 * PAD2
UNROLL = 160


def cycle_kernel(
    peers,
    slabs,
    source_far,
    conduct_far,
    out_solution,
    out_defect,
    rhs, rhs1, rhs2, scrap,
    cond, inner, gain0, hold0, gain1, hold1, gain2, hold2,
    a1, a2, a3, a4, a5, fd,
    m1, m2, m3, m4, m5,
    k1, k2, k3, k4,
    source, before, outer, conduct,
    in_send, in_recv, own_sem, load_sem, cond_load, conduct_load,
    cond_send, cond_recv,
    h_send, h_recv,
    late_send, early_send, pair_send, relay_send, sol_recv, before_recv,
    sol_own, before_own, fd_send, fd_recv, fd_own, outer_send, outer_recv,
):
    planes, rows, lanes = source.shape
    block = rows // peers
    half_planes, half_block = planes // 2, block // 2
    me, slab = lax.axis_index("tm"), lax.axis_index("space")
    mine = snake(me)
    following, preceding = snake((mine + 1) % peers), snake((mine + peers - 1) % peers)
    has_z = {1: slab < slabs - 1, -1: slab > 0, 0: None}
    has_x = {1: mine < peers - 1, -1: mine > 0, 0: None}
    beside = {1: following, -1: preceding}

    def both(first, second):
        if first is None:
            return second
        return first if second is None else first & second

    def device(dz, dx):
        where = {}
        if dx:
            where["tm"] = beside[dx]
        if dz:
            where["space"] = slab + dz
        return where

    def size_of(ref):
        pad = PAD2 if ref.shape[0] == half_planes + 2 * PAD2 else PAD
        return pad, ref.shape[0] - 2 * pad, ref.shape[1] - 2 * pad

    def over(ref, outer, inner, work):
        pad, depth, width = size_of(ref)
        z0, z1, x0, x1 = pad - outer, pad + depth + outer, pad - outer, pad + width + outer
        parts = []
        if inner is None:
            parts.append((z0, z1, list(range(x0, x1))))
        else:
            i0, i1, j0, j1 = pad - inner, pad + depth + inner, pad - inner, pad + width + inner
            parts.append((z0, i0, list(range(x0, x1))))
            parts.append((i1, z1, list(range(x0, x1))))
            parts.append((i0, i1, list(range(x0, j0)) + list(range(j1, x1))))
        over_parts(parts, work)

    def over_parts(parts, work):
        for first, last, xs in parts:
            count = last - first
            if count <= 0 or not xs:
                continue
            folds = [u for u in range(1, count + 1) if count % u == 0 and u * len(xs) <= UNROLL]
            fold = max(folds) if folds else 1
            if fold == count:
                for z in range(first, last):
                    work(z, xs)
                continue

            def step(i, _, first=first, xs=xs, fold=fold):
                for u in range(fold):
                    work(first + i * fold + u, xs)
                return 0

            lax.fori_loop(0, count // fold, step, 0)

    load_source = pltpu.make_async_copy(source_far, source, load_sem)
    load_source.start()

    def window(number):
        start, count, at = ((0, block, NEAR), (-NEAR, NEAR, 0), (block, NEAR, NEAR + block))[number]
        return pltpu.make_async_copy(
            conduct_far.at[:, pl.ds(pl.multiple_of(mine * block + start, 8), count), :],
            cond.at[pl.ds(NEAR, planes), pl.ds(at, count), :],
            cond_load.at[number],
        )

    load_whole = pltpu.make_async_copy(conduct_far, conduct, conduct_load)
    window(0).start()
    pl.when(has_x[-1])(window(1).start)
    pl.when(has_x[1])(window(2).start)

    barrier = pltpu.get_barrier_semaphore()
    for k in range(1, peers):
        pl.semaphore_signal(barrier, inc=1, device_id={"tm": me ^ k}, device_id_type=MESH)
    expected = peers - 1
    for dz in (1, -1):
        for dx in (0, 1, -1):
            here = both(has_z[dz], has_x[dx])

            @pl.when(here)
            def _(dz=dz, dx=dx):
                pl.semaphore_signal(
                    barrier, inc=1, device_id=device(dz, dx), device_id_type=MESH
                )

            expected = expected + jnp.where(here, 1, 0)
    load_source.wait()
    pl.semaphore_wait(barrier, expected)

    def rows_of(index):
        return pl.ds(pl.multiple_of(snake(index) * block, 8), block)

    def inward(peer, step, recv):
        return pltpu.make_async_remote_copy(
            src_ref=source.at[:, rows_of(peer), :],
            dst_ref=rhs.at[pl.ds(PAD, planes), pl.ds(PAD, block), step, :],
            send_sem=in_send.at[peer],
            recv_sem=in_recv.at[recv],
            device_id={"tm": peer},
            device_id_type=MESH,
        )

    order = sorted(range(1, peers), reverse=True)
    for k in order:
        inward(me ^ k, me, me).start()
    own = pltpu.make_async_copy(
        source_far.at[:, rows_of(me), :],
        rhs.at[pl.ds(PAD, planes), pl.ds(PAD, block), me, :],
        own_sem,
    )
    own.start()
    load_whole.start()
    window(0).wait()
    pl.when(has_x[-1])(window(1).wait)
    pl.when(has_x[1])(window(2).wait)

    def cond_copy(side, dz):
        return pltpu.make_async_remote_copy(
            src_ref=cond.at[pl.ds(planes, NEAR) if dz > 0 else pl.ds(NEAR, NEAR)],
            dst_ref=cond.at[pl.ds(0, NEAR) if dz > 0 else pl.ds(NEAR + planes, NEAR)],
            send_sem=cond_send.at[side],
            recv_sem=cond_recv.at[side],
            device_id={"space": slab + dz},
            device_id_type=MESH,
        )

    for side, dz in ((0, 1), (1, -1)):
        pl.when(has_z[dz])(cond_copy(side, dz).start)

    for side, dz in ((0, -1), (1, 1)):

        @pl.when(jnp.logical_not(has_z[dz]))
        def _(side=side):
            outer[side] = jnp.zeros((rows, lanes), jnp.float32)

    for ref in (rhs, m3, m5, rhs2):
        pad, deep, broad = size_of(ref)
        for dz, first in ((-1, 0), (1, pad + deep)):

            @pl.when(jnp.logical_not(has_z[dz]))
            def _(ref=ref, first=first, pad=pad):
                def clear(z, _):
                    ref[z] = jnp.zeros(ref.shape[1:], jnp.float32)
                    return 0

                lax.fori_loop(first, first + pad, clear, 0)

        for dx, first in ((-1, 0), (1, pad + broad)):

            @pl.when(jnp.logical_not(has_x[dx]))
            def _(ref=ref, first=first, pad=pad):
                def clear(z, _):
                    ref[z, first : first + pad] = jnp.zeros((pad, peers, lanes), jnp.float32)
                    return 0

                lax.fori_loop(0, ref.shape[0], clear, 0)

    for side, dz in ((0, 1), (1, -1)):
        pl.when(has_z[-dz])(cond_copy(side, dz).wait_recv)

    def fill(z, _):
        plane = slab * planes + z - PAD
        deep = (plane >= 0) & (plane < slabs * planes)
        for part in range((block + 2 * NEAR) // 8):
            at = pl.ds(8 * part, 8)
            row = mine * block - NEAR + 8 * part + lax.broadcasted_iota(jnp.int32, (8, lanes), 0)
            ok = deep & (row >= 0) & (row < rows)
            value = jnp.where(ok, cond[z - PAD + NEAR, at, :], 0.0)
            fine = jnp.where(ok, OMEGA / (1.0 + value * (2.0 * sum(FINE))), 0.0)
            middle = jnp.where(ok, OMEGA / (1.0 + value * (4.0 * sum(FINE))), 0.0)
            inner[z, at, :] = value
            gain0[z, at, :] = fine
            hold0[z, at, :] = fine * value
            gain1[z, at, :] = middle
            hold1[z, at, :] = middle * (2.0 * value)
        return 0

    lax.fori_loop(0, planes + 2 * PAD, fill, 0)

    def fill2(z, _):
        plane = slab * half_planes + z - PAD2
        deep = (plane >= 0) & (plane < slabs * half_planes)
        for part in range((block + 2 * NEAR) // 16):
            at = pl.ds(8 * part, 8)
            even, odd = pl.ds(16 * part, 8, stride=2), pl.ds(16 * part + 1, 8, stride=2)
            quad = (cond[2 * z, even, :] + cond[2 * z + 1, even, :]) + (
                cond[2 * z, odd, :] + cond[2 * z + 1, odd, :]
            )
            row = mine * half_block - PAD2 + 8 * part
            row = row + lax.broadcasted_iota(jnp.int32, (8, lanes), 0)
            ok = deep & (row >= 0) & (row < rows // 2)
            value = jnp.where(ok, 0.25 * quad, 0.0)
            gain = jnp.where(ok, OMEGA / (1.0 + value * (8.0 * sum(COARSE))), 0.0)
            gain2[z, at, :] = gain
            hold2[z, at, :] = gain * value
        return 0

    lax.fori_loop(0, half_planes + 2 * PAD2, fill2, 0)

    time = lax.broadcasted_iota(jnp.int32, (peers, lanes), 0)
    lane = lax.broadcasted_iota(jnp.int32, (peers, lanes), 1)
    not_first, not_last = lane > 0, lane < lanes - 1
    later = {count: time % count > 0 for count in (peers, peers // 2, peers // 4)}

    def pick(value, index):
        return jnp.take_along_axis(value, index, axis=0, mode="promise_in_bounds")

    def prior(value, steps):
        return jnp.where(later[steps], pltpu.roll(value, 1, 0), 0.0)

    def spread(ref, z, x, pad):
        near = PAD2 if ref.shape[1] == half_block + 2 * PAD2 else NEAR
        return jnp.broadcast_to(ref[z, pl.ds(x - pad + near, 1), :], (peers, lanes))

    def around(ref, z, xs, weight_y):
        wanted = sorted({x + step for x in xs for step in (-1, 0, 1)})
        row = {x: ref[z, x] for x in wanted}
        for x in xs:
            centre = row[x]
            across = (ref[z - 1, x] + ref[z + 1, x]) + (row[x - 1] + row[x + 1])
            along = jnp.where(not_first, pltpu.roll(centre, 1, 1), 0.0) + jnp.where(
                not_last, pltpu.roll(centre, lanes - 1, 1), 0.0
            )
            total = across + along if weight_y == 1.0 else across + weight_y * along
            yield x, centre, total

    def sweeper(new, old, first, gain, hold, steps, weight_y=1.0):
        pad = size_of(new)[0]

        def work(z, xs):
            for x, centre, total in around(old, z, xs, weight_y):
                if first is None:
                    value = (2.0 - OMEGA) * centre
                else:
                    value = (1.0 - OMEGA) * centre + first[z, x]
                value = value + spread(gain, z, x, pad) * prior(centre, steps)
                new[z, x] = value + spread(hold, z, x, pad) * total

        return work

    def starter(new, right, gain, index=None):
        pad = size_of(new)[0]

        def work(z, xs):
            for x in xs:
                value = right[z, x] if index is None else pick(right[z, x], index)
                new[z, x] = spread(gain, z, x, pad) * value

        return work

    def defecter(new, old, right, stretch, steps, paired):
        def work(z, xs):
            for x, centre, total in around(old, z, xs, 1.0):
                value = spread(inner, z, x, PAD)
                if stretch != 1.0:
                    value = stretch * value
                left = (right[z, x] + prior(centre, steps)) - centre
                left = left - value * (2.0 * sum(FINE) * centre - total)
                if paired:
                    left = pick(left, evens) + pick(left, evens + 1)
                new[z, x] = left

        return work

    half = peers // 2
    of_half, of_quarter = time % half, time % (half // 2)
    evens = 2 * of_half

    def wide(ref, into, layers, corner_layers, stage, steps):
        pad, deep, broad = size_of(ref)

        def spans(step, size, span):
            low, high = span
            if step == 0:
                return pl.ds(pad, size), pl.ds(pad, size)
            if step > 0:
                return pl.ds(pad + size - high, high - low), pl.ds(pad - high, high - low)
            return pl.ds(pad + low, high - low), pl.ds(pad + size + low, high - low)

        blocks = [(dz, dx, layers, layers) for dz, dx in ((1, 0), (-1, 0), (0, 1), (0, -1))]
        blocks += [
            (dz, dx, *ranges) for ranges in corner_layers for dz in (1, -1) for dx in (1, -1)
        ]
        out = []
        for number, (dz, dx, z_span, x_span) in enumerate(blocks):
            src_z, dst_z = spans(dz, deep, z_span)
            src_x, dst_x = spans(dx, broad, x_span)
            some = () if steps == peers else (pl.ds(0, steps),)
            copy = pltpu.make_async_remote_copy(
                src_ref=ref.at[(src_z, src_x, *some)],
                dst_ref=into.at[(dst_z, dst_x, *some)],
                send_sem=h_send.at[stage, number],
                recv_sem=h_recv.at[stage, number],
                device_id=device(dz, dx),
                device_id_type=MESH,
            )
            sends = both(has_z[dz], has_x[dx])
            arrives = both(has_z[-dz], has_x[-dx])
            out.append((sends, arrives, copy))
        return out

    started = {}

    def send(ref, into, layers, corner_layers, stage, steps):
        started[stage] = wide(ref, into, layers, corner_layers, stage, steps)
        for sends, _, copy in started[stage]:
            pl.when(sends)(copy.start)

    def square(depth):
        return (((0, depth), (0, depth)),)

    def receive(stage):
        for _, arrives, copy in started[stage]:
            pl.when(arrives)(copy.wait_recv)

    def pieces_of(ref, edge):
        _, deep, broad = size_of(ref)
        return (
            (edge, deep - 2 * edge, edge, broad - 2 * edge),
            (0, edge, 0, broad),
            (deep - edge, edge, 0, broad),
            (edge, deep - 2 * edge, 0, edge),
            (edge, deep - 2 * edge, broad - edge, edge),
        )

    parts = pieces_of(a5, 2)
    pair, odd = me // 2, me % 2
    partner = me + 1 - 2 * odd
    others = sorted(range(1, peers // 2), reverse=True)

    def on_parity(work):
        pl.when(odd == 0)(functools.partial(work, 0))
        pl.when(odd == 1)(functools.partial(work, 1))

    def cut(step, piece):
        z, deep, x, broad = parts[piece]
        return a5.at[pl.ds(z + PAD, deep), pl.ds(x + PAD, broad), step, :]

    def laid(ref, owner, piece):
        z, deep, x, broad = parts[piece]
        return ref.at[pl.ds(z, deep), pl.ds(snake(owner) * block + x, broad), :]

    def place(parity):
        return (before, before_recv) if parity else (out_solution, sol_recv)

    def remote(src, dst, send_sem, recv_sem, peer):
        return pltpu.make_async_remote_copy(
            src_ref=src,
            dst_ref=dst,
            send_sem=send_sem,
            recv_sem=recv_sem,
            device_id={"tm": peer},
            device_id_type=MESH,
        )

    def late(piece, group, owner, peer):
        return remote(
            cut(peer, piece), laid(out_solution, owner, piece),
            late_send.at[piece, group], sol_recv.at[piece, owner], peer,
        )

    def early(parity, piece, group, owner, step, peer):
        into, arrived = place(parity)
        return remote(
            cut(step, piece), laid(into, owner, piece),
            early_send.at[piece, group], arrived.at[piece, owner], peer,
        )

    def to_partner(parity, piece, owner):
        into, arrived = place(1 - parity)
        return remote(
            cut(2 * pair, piece), laid(into, owner, piece),
            pair_send.at[piece], arrived.at[piece, owner], partner,
        )

    def relay(parity, piece, group, owner):
        source_of = place(parity)[0]
        into, arrived = place(1 - parity)
        return remote(
            laid(source_of, owner, piece), laid(into, owner, piece),
            relay_send.at[piece, group], arrived.at[piece, owner], partner,
        )

    def own_solution(piece):
        return pltpu.make_async_copy(cut(me, piece), laid(out_solution, me, piece), sol_own.at[piece])

    def own_before(piece):
        return pltpu.make_async_copy(cut(me - 1, piece), laid(before, me, piece), before_own.at[piece])

    def ship(piece):
        for k in others:
            group = pair ^ k
            late(piece, group, me, 2 * group + 1).start()

            def begin(parity, group=group):
                early(parity, piece, group, me, 2 * group, 2 * group + parity).start()

            on_parity(begin)

        def near(parity):
            to_partner(parity, piece, me).start()
            if parity:
                own_before(piece).start()
            else:
                late(piece, pair, me, partner).start()

        on_parity(near)
        own_solution(piece).start()

    def fd_copy(group, owner):
        return remote(
            fd.at[pl.ds(PAD, planes), pl.ds(PAD, block), 2 * group, :],
            out_defect.at[:, pl.ds(pl.multiple_of(snake(owner) * block, 8), block), :],
            fd_send.at[group], fd_recv.at[owner], 2 * group,
        )

    own_fd = pltpu.make_async_copy(
        fd.at[pl.ds(PAD, planes), pl.ds(PAD, block), me, :], out_defect.at[:, rows_of(me), :], fd_own
    )

    def outer_copy(side, dz):
        return pltpu.make_async_remote_copy(
            src_ref=out_solution.at[planes - 1 if dz > 0 else 0],
            dst_ref=outer.at[0 if dz > 0 else 1],
            send_sem=outer_send.at[side],
            recv_sem=outer_recv.at[side],
            device_id={"space": slab + dz},
            device_id_type=MESH,
        )

    own.wait()
    for k in order:
        inward(me, me ^ k, me ^ k).wait_recv()

    send(rhs, rhs, (0, 2), square(1), 0, peers)
    send(rhs, rhs, (2, 4), (((0, 1), (1, 3)), ((1, 3), (0, 2))), 1, peers)
    first = starter(a1, rhs, gain0)
    second = sweeper(a2, a1, None, gain0, hold0, peers)
    third = defecter(rhs1, a2, rhs, 1.0, peers, True)
    over(a1, 0, None, first)
    over(a2, -1, None, second)
    over(rhs1, -2, None, third)
    receive(0)
    top, left = PAD + planes, PAD + block
    inside = list(range(PAD, left))
    flank = [PAD - 2, PAD - 1, left, left + 1]
    over_parts(
        [(PAD - 2, PAD, inside), (top, top + 2, inside), (PAD, top, flank)]
        + [(z, z + 1, [PAD - 1, left]) for z in (PAD - 1, top)],
        first,
    )
    middle_rows = [PAD - 1, *inside, left]
    over_parts(
        [(PAD - 1, PAD, inside), (PAD, PAD + 1, middle_rows)]
        + [(top - 1, top, middle_rows), (top, top + 1, inside)]
        + [(PAD + 1, top - 1, [PAD - 1, PAD, left - 1, left])],
        second,
    )
    over(rhs1, 0, -2, third)
    fourth = starter(m1, rhs1, gain1)
    fifth = sweeper(m2, m1, None, gain1, hold1, half)
    sixth = defecter(scrap, m2, rhs1, 2.0, half, False)
    over(m1, 0, None, fourth)
    over(m2, -1, None, fifth)
    over(scrap, -2, None, sixth)
    receive(1)
    for z in (PAD - 2, PAD - 1, top, top + 1):
        first(z, flank)
    over(a1, 4, 2, first)
    for z in (PAD - 1, top):
        second(z, [PAD - 1, left])
    over(a2, 3, 1, second)
    over(rhs1, 2, 0, third)
    over(m1, 2, 0, fourth)
    over(m2, 1, -1, fifth)
    over(scrap, 0, -2, sixth)

    pairs = 2 * of_quarter

    def restrict(z, _):
        for x in range(half_block):
            zz, xx = 2 * z + PAD, 2 * x + PAD
            quad = (scrap[zz, xx] + scrap[zz + 1, xx]) + (
                scrap[zz, xx + 1] + scrap[zz + 1, xx + 1]
            )
            rhs2[z + PAD2, x + PAD2] = 0.25 * (pick(quad, pairs) + pick(quad, pairs + 1))
        return 0

    lax.fori_loop(0, half_planes, restrict, 0)
    send(rhs2, rhs2, (0, 4), square(4), 3, half // 2)
    send(m2, m3, (0, 2), square(1), 4, half)
    start = starter(k1, rhs2, gain2, of_quarter)
    second, third, fourth = (
        sweeper(new, old, first, gain2, hold2, half // 2, 4.0)
        for new, old, first in ((k2, k1, None), (k3, k2, k1), (k4, k3, k1))
    )
    over(k1, 0, None, start)
    over(k2, -1, None, second)
    receive(3)
    over(k1, 4, 0, start)
    over(k2, 3, -1, second)
    over(k3, 2, None, third)
    over(k4, 1, None, fourth)

    halved = of_half // 2

    def prolonger(received):
        def work(z, xs):
            for x in xs:
                value = pick(k4[z, x], halved)
                for dz in range(2):
                    for dx in range(2):
                        at = (2 * (z - PAD2) + dz + PAD, 2 * (x - PAD2) + dx + PAD)
                        base = pick(m3[at], of_half) if received else m2[at]
                        m3[at] = base + value

        return work

    over(k4, 0, None, prolonger(False))
    receive(4)
    over(k4, 1, 0, prolonger(True))
    over(m4, 1, None, sweeper(m4, m3, m1, gain1, hold1, half))
    over(m5, 0, None, sweeper(m5, m4, m1, gain1, hold1, half))
    send(m5, m5, (0, 3), square(2), 5, half)

    def joiner(base):
        def work(z, xs):
            for x in xs:
                a3[z, x] = base[z, x] + pick(m5[z, x], time // 2)

        return work

    fourth = sweeper(a4, a3, a1, gain0, hold0, peers)
    fifth = sweeper(a5, a4, a1, gain0, hold0, peers)
    last = defecter(fd, a5, rhs, 1.0, peers, False)
    over(a3, 0, None, joiner(a2))
    over(a4, -1, None, fourth)
    over(a5, -2, None, fifth)
    ship(0)
    over(fd, -3, None, last)
    receive(5)
    over(a3, 3, 0, joiner(a2))
    over(a4, 2, -1, fourth)
    over(a5, 1, -2, fifth)
    for piece in range(1, 5):
        ship(piece)
    over(fd, 0, -3, last)
    for k in others:
        fd_copy(pair ^ k, me).start()
    pl.when(odd == 0)(own_fd.start)
    pl.when(odd == 1)(fd_copy(pair, me).start)

    def forward(parity):
        for piece in (0, 1, 2, None, 3, 4):
            if piece is None:
                if parity:
                    for edge, side, dz in ((1, 1, -1), (2, 0, 1)):
                        own_solution(edge).wait()
                        for k in range(1, peers):
                            late(edge, 0, me ^ k, me).wait_recv()
                        pl.when(has_z[dz])(outer_copy(side, dz).start)
                continue
            for k in reversed(others):
                owner = 2 * (pair ^ k) + parity
                early(parity, piece, 0, owner, 2 * pair, me).wait_recv()
                relay(parity, piece, pair ^ k, owner).start()

    on_parity(forward)

    @pl.when(odd == 1)
    def _():
        for piece in (0, 3, 4):
            own_solution(piece).wait()
            for k in range(1, peers):
                late(piece, 0, me ^ k, me).wait_recv()
        load_whole.wait()
        row = lax.broadcasted_iota(jnp.int32, (rows, lanes), 0)
        column = lax.broadcasted_iota(jnp.int32, (rows, lanes), 1)
        for z in (*range(1, planes - 1), None, 0, planes - 1):
            if z is None:
                for side, dz in ((0, 1), (1, -1)):
                    pl.when(has_z[-dz])(outer_copy(side, dz).wait_recv)
                continue
            centre = out_solution[z]
            across = (out_solution[z - 1] if z else outer[0]) + (
                out_solution[z + 1] if z < planes - 1 else outer[1]
            )
            across = across + (
                jnp.where(row > 0, pltpu.roll(centre, 1, 0), 0.0)
                + jnp.where(row < rows - 1, pltpu.roll(centre, rows - 1, 0), 0.0)
            )
            along = jnp.where(column > 0, pltpu.roll(centre, 1, 1), 0.0) + jnp.where(
                column < lanes - 1, pltpu.roll(centre, lanes - 1, 1), 0.0
            )
            left = source[z] - centre
            out_defect[z] = left - conduct[z] * (2.0 * sum(FINE) * centre - (across + along))
        for piece in range(5):
            own_before(piece).wait()
            to_partner(0, piece, partner).wait_recv()
            for k in others:
                relay(0, piece, 0, 2 * (pair ^ k)).wait_recv()
        for z in range(planes):
            out_defect[z] = out_defect[z] + before[z]
        for side, dz in ((0, 1), (1, -1)):
            pl.when(has_z[dz])(outer_copy(side, dz).wait_send)

    @pl.when(odd == 0)
    def _():
        load_whole.wait()
        own_fd.wait()
        for piece in range(5):
            own_solution(piece).wait()
            late(piece, pair, me, partner).wait_send()
            to_partner(1, piece, partner).wait_recv()
            for k in others:
                relay(1, piece, 0, 2 * (pair ^ k) + 1).wait_recv()
        for k in range(1, peers):
            fd_copy(pair, me ^ k).wait_recv()

    for copies in started.values():
        for sends, _, copy in copies:
            pl.when(sends)(copy.wait_send)
    for side, dz in ((0, 1), (1, -1)):
        pl.when(has_z[dz])(cond_copy(side, dz).wait_send)
    for k in order:
        inward(me ^ k, me, me).wait_send()
    for k in others:
        fd_copy(pair ^ k, me).wait_send()
    pl.when(odd == 1)(fd_copy(pair, me).wait_send)

    def finish(parity):
        for piece in range(5):
            to_partner(parity, piece, me).wait_send()
            for k in others:
                late(piece, pair ^ k, me, me).wait_send()
                early(parity, piece, pair ^ k, me, 0, me).wait_send()
                relay(parity, piece, pair ^ k, 2 * (pair ^ k) + parity).wait_send()

    on_parity(finish)


def fused_body(peers, slabs, source, conductivity):
    _, planes, rows, lanes = source.shape
    block = rows // peers

    def field(depth, width):
        return pltpu.VMEM((depth, width, peers, lanes), jnp.float32)

    def table(depth, width):
        return pltpu.VMEM((depth, width, lanes), jnp.float32)

    large = field(planes + 2 * PAD, block + 2 * PAD)
    small = field(planes // 2 + 2 * PAD2, block // 2 + 2 * PAD2)
    fine = table(planes + 2 * PAD, block + 2 * NEAR)
    coarse = table(planes // 2 + 2 * PAD2, block // 2 + 2 * PAD2)
    dma = pltpu.SemaphoreType.DMA
    anywhere = pl.BlockSpec(memory_space=pl.ANY)
    local = pl.BlockSpec(memory_space=pltpu.VMEM)
    shape = pltpu.VMEM((planes, rows, lanes), jnp.float32)
    solution, final_defect = pl.pallas_call(
        functools.partial(cycle_kernel, peers, slabs),
        out_shape=(shape, shape),
        in_specs=[anywhere, anywhere],
        out_specs=(local, local),
        scratch_shapes=[
            large, large, small, large,
            table(planes + 2 * NEAR, block + 2 * NEAR),
            fine, fine, fine, fine, fine, coarse, coarse,
            large, large, large, large, large, large,
            large, large, large, large, large,
            small, small, small, small,
            pltpu.VMEM((planes, rows, lanes), jnp.float32),
            pltpu.VMEM((planes, rows, lanes), jnp.float32),
            pltpu.VMEM((2, rows, lanes), jnp.float32),
            pltpu.VMEM((planes, rows, lanes), jnp.float32),
            dma((peers,)), dma((peers,)), dma, dma, dma((3,)), dma,
            dma((2,)), dma((2,)),
            dma((6, 12)), dma((6, 12)),
            dma((5, peers // 2)), dma((5, peers // 2)), dma((5,)), dma((5, peers // 2)),
            dma((5, peers)), dma((5, peers)), dma((5,)), dma((5,)),
            dma((peers // 2,)), dma((peers,)), dma, dma((2,)), dma((2,)),
        ],
        compiler_params=pltpu.CompilerParams(
            collective_id=0, has_side_effects=True, vmem_limit_bytes=56 * 1024 * 1024
        ),
    )(source[0], conductivity)
    return (solution[None], final_defect[None])


def solution(mesh):
    peers, slabs = mesh.shape["tm"], mesh.shape["space"]

    def chosen(source, conductivity):
        steps, planes, rows, lanes = source.shape
        if fits(steps * peers, peers, slabs, planes, rows, lanes):
            return fused_body(peers, slabs, source, conductivity)
        return body(source, conductivity)

    return jax.shard_map(
        chosen,
        mesh=mesh,
        in_specs=(P("tm", "space", None, None), P("space", None, None)),
        out_specs=(P("tm", "space", None, None), P("tm", "space", None, None)),
        check_vma=False,
    )
```
